256 devices in a mesh: kpt: 2 (over y), ga: 128 (over x, z, core).
Axes of the slice: x: 4, y: 2, z: 16, core: 2. Of those that a mesh axis runs over, the one named last changes fastest.
The devices are a block of a 4x16x16 slice.
Arguments:
- miller_index: int32 [3, 98304], P(None, 'ga'), may hold values from -12 to 12
- kpoint: float32 [6], P('kpt'), parts along dimension 0, may hold values from -0.5 to 0.5
- waves: bfloat16 [2, 256, 98304], P(None, 'kpt', 'ga'), parts along dimension 1, may hold values from -6 to 6
- species: int32 [128], replicated, may hold values from 0 to 3
- counts: int32 [128], replicated, may hold values from 1 to 8
- positions: int32 [3, 128], replicated, may hold values from 0 to 63
- radial_coef: float32 [4, 8, 16], replicated, may hold values from -4 to 4
- coupling: float32 [128, 8, 8], replicated, as said below
Outputs:
- applied: bfloat16 [2, 256, 98304], P(None, 'kpt', 'ga'), parts along dimension 1
- energy: float32 [256], P('kpt'), parts along dimension 0
The draws below stay inside these ranges and needn't reach their ends.
There are 2 independent parts, one for each index of `kpt`. The reference program is written for one: setup_inputs(seed, part) draws one part's arguments, and reference() takes and returns one part's arrays. A program takes and returns all parts, laid end to end along the dimension named above; an argument that names none is the same for every part. Nothing has to cross between parts.
Inputs may be any that keep to these rules, and one draw needn't show every extreme that they name: `coupling`: symmetric in its last two dimensions.
All inputs are finite; a program needn't handle non-finite values.
Results may differ from the reference program's by a relative error of at most 0.0062.
Values may be sent and summed in bfloat16 or wider, within the bound.
No kernel may reach another device: no remote copies, remote signals or barrier semaphores. Data moves between devices by JAX's collectives and lax.ppermute only.
A program may use at most 64 MiB of HBM per device.

```python
import math
import jax
import jax.numpy as jnp
from jax import lax

BANDS = 128
PROJ = 8
NSPEC = 4
NRAD = 16
MGRID = 64
HMAX = 12
ATOM_BLOCK = 16
NAT = 128
PW = 98304
NPROJ = 1024
NBLK = 8


def draw_coupling(key, part):
    first, second, third = jax.random.split(key, 3)
    raw = jax.random.normal(first, (NAT, PROJ, PROJ), jnp.float32)
    symmetric = 0.6 * (raw + jnp.swapaxes(raw, 1, 2))
    diagonal = jax.random.uniform(second, (NAT, PROJ), jnp.float32, 3.0, 6.0)
    signs = jnp.where(jax.random.bernoulli(third, 0.7, (NAT, PROJ)), 1.0, -1.0)
    return symmetric + jnp.eye(PROJ, dtype=jnp.float32)[None] * (diagonal * signs)[:, :, None]


def touch_ends(values, key, low, high):
    dims = values.shape
    index_at = [jax.random.randint(jax.random.fold_in(key, axis), (), 0, dims[axis]) for axis in range(len(dims))]
    values = values.at[tuple(index_at)].set(low)
    longest = dims.index(max(dims))
    index_at[longest] = (index_at[longest] + 1) % dims[longest]
    return values.at[tuple(index_at)].set(high)


def level_of(stream_key, dims, shards, least, top_value):
    loudness, own = 1.0, jax.random.fold_in(stream_key, 6)
    for position, parts in shards:
        steps = jnp.exp(jax.random.uniform(jax.random.fold_in(own, position), (parts,), jnp.float32, least / len(shards), top_value / len(shards)))
        loudness = loudness * jnp.repeat(steps, dims[position] // parts).reshape([-1 if axis == position else 1 for axis in range(len(dims))])
    return loudness


def normal_values(stream_key, extent, deviation, bound, shards=(), kind=jnp.bfloat16):
    values = deviation * jax.random.normal(stream_key, extent, jnp.float32)
    if shards:
        values = values * level_of(stream_key, extent, shards, -0.22, 0.18)
    return jnp.clip(values, -bound, bound).astype(kind)


def setup_inputs(seed: int = 0, part: int = 0) -> dict:
    splits = jax.random.split(jax.random.key(seed), 9)
    part_splits = jax.random.split(jax.random.fold_in(splits[8], part), 9)
    miller_index = touch_ends(jax.random.randint(splits[0], (3, PW), -HMAX, HMAX + 1), jax.random.fold_in(splits[0], 1), -HMAX, HMAX).astype(jnp.int32)
    kpoint = jnp.clip(jax.random.uniform(part_splits[1], (3,), jnp.float32, -0.5, 0.5), -0.5, 0.5)
    waves = normal_values(part_splits[2], (2, BANDS, PW), 1.0, 6.0, ((2, 128),))
    species = touch_ends(jax.random.randint(splits[3], (NAT,), 0, NSPEC), jax.random.fold_in(splits[3], 1), 0, NSPEC - 1).astype(jnp.int32)
    counts = touch_ends(jax.random.randint(splits[4], (NAT,), 1, PROJ + 1), jax.random.fold_in(splits[4], 1), 1, PROJ).astype(jnp.int32)
    positions = touch_ends(jax.random.randint(splits[5], (3, NAT), 0, MGRID), jax.random.fold_in(splits[5], 1), 0, MGRID - 1).astype(jnp.int32)
    radial_coef = normal_values(splits[6], (NSPEC, PROJ, NRAD), 1.0, 4.0, (), jnp.float32)
    coupling = draw_coupling(jax.random.fold_in(splits[8], 71), part)
    return dict(miller_index=miller_index, kpoint=kpoint, waves=waves, species=species, counts=counts, positions=positions, radial_coef=radial_coef, coupling=coupling)


def prepare(miller_index, kpoint, terms):
    shifted = miller_index.astype(jnp.float32) + kpoint[:, None]
    squared = lax.optimization_barrier(jnp.sum(shifted * shifted, axis=0))
    widths = 0.001 * 1.5 ** jnp.arange(terms).astype(jnp.float32)
    basis = jnp.exp(-widths[:, None] * squared[None, :])
    angular = jnp.concatenate([jnp.ones_like(squared)[None], shifted / jnp.sqrt(squared + 1.0)[None]], 0)
    angular = jnp.concatenate([angular, angular], 0)
    return (basis, angular)

def projectors(first, miller_index, kpoint, basis, angular, species, counts, positions, radial_coef, scaling):
    kinds = lax.dynamic_slice_in_dim(species, first, ATOM_BLOCK)
    numbers = lax.dynamic_slice_in_dim(counts, first, ATOM_BLOCK)
    places = lax.dynamic_slice_in_dim(positions, first, ATOM_BLOCK, 1)
    selector = (kinds[:, None] == jnp.arange(radial_coef.shape[0]).astype(jnp.int32)[None, :]).astype(jnp.float32)
    chosen = jnp.einsum('as,sjr->ajr', selector, radial_coef, precision=lax.Precision.HIGHEST)
    radial = jnp.einsum('ajr,rg->ajg', chosen, basis, precision=lax.Precision.HIGHEST)
    active = (jnp.arange(PROJ).astype(jnp.int32)[None, :] < numbers[:, None]).astype(jnp.float32)
    amplitude = radial * angular[None] * active[:, :, None] * scaling
    winding = jnp.mod(lax.optimization_barrier(jnp.sum(miller_index[:, None, :] * places[:, :, None], axis=0)), MGRID)
    offset = lax.optimization_barrier(jnp.sum(kpoint[:, None] * places.astype(jnp.float32), axis=0))
    phase = 2.0 * math.pi / MGRID * (winding.astype(jnp.float32) + offset[:, None])
    planes = miller_index.shape[1]
    real_part = (amplitude * jnp.cos(phase)[:, None, :]).astype(jnp.bfloat16).reshape(ATOM_BLOCK * PROJ, planes)
    imag_part = (-amplitude * jnp.sin(phase)[:, None, :]).astype(jnp.bfloat16).reshape(ATOM_BLOCK * PROJ, planes)
    return (real_part, imag_part)

def reference(miller_index, kpoint, waves, species, counts, positions, radial_coef, coupling):
    scaling = 1.0 / math.sqrt(PW)
    basis, angular = prepare(miller_index, kpoint, radial_coef.shape[2])
    wave_re = waves[0].astype(jnp.float32)
    wave_im = waves[1].astype(jnp.float32)
    width = ATOM_BLOCK * PROJ

    def build(index):
        return projectors(index * ATOM_BLOCK, miller_index, kpoint, basis, angular, species, counts, positions, radial_coef, scaling)

    def measure(index):
        real_part, imag_part = build(index)
        real_part = real_part.astype(jnp.float32)
        imag_part = imag_part.astype(jnp.float32)
        over_re = jnp.einsum('sg,bg->sb', real_part, wave_re) + jnp.einsum('sg,bg->sb', imag_part, wave_im)
        over_im = jnp.einsum('sg,bg->sb', real_part, wave_im) - jnp.einsum('sg,bg->sb', imag_part, wave_re)
        return jnp.stack([over_re, over_im])
    table = lax.map(measure, jnp.arange(NBLK).astype(jnp.int32))
    table = jnp.transpose(table, (1, 0, 2, 3)).reshape(2, NAT, PROJ, BANDS)
    weighted = jnp.einsum('aij,cajb->caib', coupling, table, precision=lax.Precision.HIGHEST)
    energy = lax.optimization_barrier(jnp.sum(table * weighted, axis=(0, 1, 2))) / NPROJ
    rounded = weighted.reshape(2, NPROJ, BANDS).astype(jnp.bfloat16)

    def accumulate(total, index):
        real_part, imag_part = build(index)
        real_part = real_part.astype(jnp.float32)
        imag_part = imag_part.astype(jnp.float32)
        rows = lax.dynamic_slice_in_dim(rounded, (index * width).astype(jnp.int32), width, 1).astype(jnp.float32)
        out_re = jnp.einsum('sb,sg->bg', rows[0], real_part) - jnp.einsum('sb,sg->bg', rows[1], imag_part)
        out_im = jnp.einsum('sb,sg->bg', rows[1], real_part) + jnp.einsum('sb,sg->bg', rows[0], imag_part)
        return (total + jnp.stack([out_re, out_im]), None)
    output, unused = lax.scan(accumulate, jnp.zeros((2, BANDS, PW), jnp.float32), jnp.arange(NBLK).astype(jnp.int32))
    return (output.astype(jnp.bfloat16), energy)
```

```python
import functools
import math

import jax
import jax.numpy as jnp
import numpy as np
from jax import lax
from jax.experimental import pallas as pl
from jax.experimental.pallas import tpu as pltpu
from jax.sharding import Mesh
from jax.sharding import PartitionSpec as P

PROJ = 8
MGRID = 64
GA = ("x", "zh", "zl", "c")
NEAR = ("x", "zl")
FAR = "zh"
CORE = "c"
EXTRA = 8


def turn_series(degree=9):
    nodes = 0.125 + 0.125 * np.cos(np.pi * (np.arange(64) + 0.5) / 64)
    root = np.sqrt(nodes)
    fit = np.polynomial.chebyshev.Chebyshev.fit
    poly = np.polynomial.Polynomial
    cosine = fit(nodes, np.cos(2 * np.pi * root), degree, domain=[0, 0.25]).convert(kind=poly)
    sine = fit(nodes, np.sin(2 * np.pi * root) / root, degree, domain=[0, 0.25]).convert(kind=poly)
    return [float(v) for v in cosine.coef], [float(v) for v in sine.coef]


COSINE, SINE = turn_series()


def series(coefficients, y):
    total = jnp.full_like(y, coefficients[-1])
    for value in coefficients[-2::-1]:
        total = total * y + value
    return total


def nearest(x):
    return jnp.floor(x + 0.5)


def build_kernel(
    scaling,
    half_ref,
    kpoint_ref,
    species_ref,
    counts_ref,
    miller_ref,
    waves_ref,
    positions_ref,
    radial_ref,
    over_ref,
    real_ref,
    imag_ref,
    amp_ref,
    cos_ref,
    sin_ref,
):
    f32, bf16 = jnp.float32, jnp.bfloat16
    terms = radial_ref.shape[1]
    planes = miller_ref.shape[1]
    slots = real_ref.shape[0]
    atoms = slots // PROJ
    kinds = radial_ref.shape[0] // PROJ
    half = half_ref[0]

    miller = miller_ref[...].astype(f32)
    shifted = [miller[c : c + 1] + kpoint_ref[c] for c in range(3)]
    squared = shifted[0] * shifted[0] + shifted[1] * shifted[1] + shifted[2] * shifted[2]
    order = lax.broadcasted_iota(jnp.int32, (terms, planes), 0)
    widths = jnp.zeros((terms, planes), f32)
    for r in range(terms):
        widths = jnp.where(order == r, 0.001 * 1.5**r, widths)
    basis = jnp.exp(-widths * squared)
    radial = jnp.dot(
        radial_ref[...], basis, precision=lax.Precision.HIGHEST, preferred_element_type=f32
    )
    scale = 1.0 / jnp.sqrt(squared + 1.0)
    row = lax.broadcasted_iota(jnp.int32, (PROJ, planes), 0) % 4
    angular = jnp.where(row == 0, 1.0, jnp.where(row == 1, shifted[0] * scale, 0.0))
    angular = jnp.where(row == 2, shifted[1] * scale, angular)
    angular = jnp.where(row == 3, shifted[2] * scale, angular) * scaling
    for s in range(kinds):
        amp_ref[s * PROJ : (s + 1) * PROJ, :] = radial[s * PROJ : (s + 1) * PROJ] * angular

    places = positions_ref[...].astype(f32)
    third = lax.broadcasted_iota(jnp.int32, (3, 128), 0)
    point = jnp.where(third == 0, kpoint_ref[0], jnp.where(third == 1, kpoint_ref[1], kpoint_ref[2]))
    inner = (((0,), (0,)), ((), ()))
    winding = lax.dot_general(
        places.astype(bf16), miller.astype(bf16), inner, preferred_element_type=f32
    )
    offset = lax.dot_general(
        places, point, inner, precision=lax.Precision.HIGHEST, preferred_element_type=f32
    )
    winding = winding * (1.0 / MGRID)
    offset = offset * (1.0 / MGRID)
    winding = winding - nearest(winding)
    offset = offset - nearest(offset)
    cos_ref[...] = winding + jnp.concatenate([offset] * (planes // 128), 1)

    first = pl.multiple_of(half * atoms, atoms)
    turns = cos_ref[pl.ds(first, atoms), :]
    turns = turns - nearest(turns)
    square = turns * turns
    cosine = series(COSINE, square)
    sine = series(SINE, square) * -turns
    cos_ref[0:atoms, :] = cosine
    sin_ref[...] = sine

    slot = lax.broadcasted_iota(jnp.int32, (PROJ, planes), 0)
    per = 4

    def build(step, carry):
        real, imag = [], []
        for k in range(per):
            at = step * per + k
            kind = species_ref[first + at]
            number = counts_ref[first + at]
            amp = amp_ref[pl.ds(pl.multiple_of(kind * PROJ, PROJ), PROJ), :]
            amp = jnp.where(slot < number, amp, 0.0)
            real.append(amp * cos_ref[pl.ds(at, 1), :])
            imag.append(amp * sin_ref[pl.ds(at, 1), :])
        rows = pl.ds(pl.multiple_of(step * per * PROJ, per * PROJ), per * PROJ)
        real_ref[rows, :] = jnp.concatenate(real, 0).astype(bf16)
        imag_ref[rows, :] = jnp.concatenate(imag, 0).astype(bf16)
        return carry

    lax.fori_loop(0, atoms // per, build, 0)

    waves = waves_ref[...]
    bands = waves.shape[0] // 2
    turned = jnp.concatenate([waves[bands:], -waves[:bands]], 0)
    outer = (((1,), (1,)), ((), ()))
    over_ref[...] = lax.dot_general(
        real_ref[...], waves, outer, preferred_element_type=f32
    ) + lax.dot_general(imag_ref[...], turned, outer, preferred_element_type=f32)


def build_half(half, scaling, kpoint, species, counts, miller, waves, positions, radial):
    planes = miller.shape[1]
    atoms = species.shape[0] // 2
    slots = atoms * PROJ
    smem = pl.BlockSpec(memory_space=pltpu.SMEM)
    vmem = pl.BlockSpec(memory_space=pltpu.VMEM)
    shape = jax.ShapeDtypeStruct
    return pl.pallas_call(
        functools.partial(build_kernel, scaling),
        out_shape=(
            shape((slots, waves.shape[0]), jnp.float32),
            shape((slots, planes), jnp.bfloat16),
            shape((slots, planes), jnp.bfloat16),
        ),
        in_specs=[smem] * 4 + [vmem] * 4,
        out_specs=(vmem,) * 3,
        scratch_shapes=[
            pltpu.VMEM((radial.shape[0], planes), jnp.float32),
            pltpu.VMEM((2 * atoms, planes), jnp.float32),
            pltpu.VMEM((atoms, planes), jnp.float32),
        ],
        cost_estimate=pl.CostEstimate(
            flops=8 * slots * planes * 128, bytes_accessed=4 * 1024 * 1024, transcendentals=0
        ),
        compiler_params=pltpu.CompilerParams(vmem_limit_bytes=32 * 1024 * 1024),
        name="build",
    )(half, kpoint, species, counts, miller, waves, positions, radial)


def fold_kernel(parts_ref, out_ref):
    total = jnp.sum(parts_ref[...].astype(jnp.float32), axis=0).astype(out_ref.dtype)
    for k in range(out_ref.shape[0]):
        out_ref[k] = total


def fold(parts, copies):
    return pl.pallas_call(
        fold_kernel,
        out_shape=jax.ShapeDtypeStruct((copies, *parts.shape[1:]), parts.dtype),
        in_specs=[pl.BlockSpec(memory_space=pltpu.VMEM)],
        out_specs=pl.BlockSpec(memory_space=pltpu.VMEM),
        name="fold",
    )(parts)


def weigh_kernel(chunk_ref, parts_ref, coupling_ref, out_ref):
    f32, bf16 = jnp.float32, jnp.bfloat16
    over = jnp.sum(parts_ref[...].astype(f32), axis=0)
    rows, both = over.shape
    bands = both // 2
    matrix = coupling_ref[pl.ds(pl.multiple_of(chunk_ref[0] * rows, rows), rows), :]
    weighted = []
    for k in range(rows // PROJ):
        block = over[k * PROJ : (k + 1) * PROJ]
        part = matrix[k * PROJ : (k + 1) * PROJ]
        total = part[:, 0:1] * block[0:1]
        for j in range(1, PROJ):
            total = total + part[:, j : j + 1] * block[j : j + 1]
        weighted.append(total)
    weighted = jnp.concatenate(weighted, 0)
    energy = jnp.sum(over * weighted, axis=0, keepdims=True)
    energy = energy[:, :bands] + energy[:, bands:]
    high = energy.astype(bf16).astype(f32)
    share = jnp.concatenate([high, energy - high], 1)
    index = lax.broadcasted_iota(jnp.int32, (EXTRA, both), 0)
    share = jnp.where(index == 0, share, 0.0)
    whole = jnp.concatenate([weighted, share], 0).astype(bf16)
    for k in range(out_ref.shape[0]):
        out_ref[k] = whole


def weigh(chunk, parts, coupling, copies):
    rows, both = parts.shape[1:]
    smem = pl.BlockSpec(memory_space=pltpu.SMEM)
    vmem = pl.BlockSpec(memory_space=pltpu.VMEM)
    return pl.pallas_call(
        weigh_kernel,
        out_shape=jax.ShapeDtypeStruct((copies, rows + EXTRA, both), jnp.bfloat16),
        in_specs=[smem, vmem, vmem],
        out_specs=vmem,
        name="weigh",
    )(chunk, parts, coupling)


def spread(table_ref, real_ref, imag_ref):
    copies, rows, both = table_ref.shape
    rows = rows - EXTRA
    bands = both // 2
    table = table_ref[:, 0:rows, :].reshape(copies * rows, both)
    turned = jnp.concatenate([-table[:, bands:], table[:, :bands]], 1)
    inner = (((0,), (0,)), ((), ()))
    return lax.dot_general(
        table, real_ref[...], inner, preferred_element_type=jnp.float32
    ) + lax.dot_general(turned, imag_ref[...], inner, preferred_element_type=jnp.float32)


def share_of(table_ref):
    both = table_ref.shape[2]
    rows = table_ref.shape[1] - EXTRA
    share = jnp.sum(table_ref[:, rows:, :].astype(jnp.float32), axis=(0, 1), keepdims=True)[0]
    return share[:, : both // 2] + share[:, both // 2 :]


def first_kernel(table_ref, real_ref, imag_ref, out_ref):
    out_ref[...] = spread(table_ref, real_ref, imag_ref)


def last_kernel(slots, own_ref, table_ref, real_ref, imag_ref, total_ref, out_ref, energy_ref):
    out_ref[...] = (total_ref[...] + spread(table_ref, real_ref, imag_ref)).astype(out_ref.dtype)
    energy_ref[...] = (share_of(own_ref) + share_of(table_ref)) / slots


def on_device(miller_index, kpoint, waves, species, counts, positions, radial_coef, coupling):
    planes = waves.shape[2]
    bands = waves.shape[1]
    scaling = 1.0 / math.sqrt(planes * lax.axis_size(GA))
    slots = coupling.shape[0] * PROJ
    near = lax.axis_size(NEAR)
    far = lax.axis_size(FAR)
    rows = slots // (2 * near)
    vmem = pl.BlockSpec(memory_space=pltpu.VMEM)
    core = lax.axis_index(CORE)
    swap = [(0, 1), (1, 0)]
    flat = waves.reshape(2 * bands, planes)
    radial = radial_coef.reshape(-1, radial_coef.shape[2])

    def build(half):
        return build_half(
            half.reshape(1), scaling, kpoint, species, counts, miller_index, flat, positions, radial
        )

    sent, real_other, imag_other = build(1 - core)
    come = lax.ppermute(sent, CORE, swap)
    kept, real_own, imag_own = build(core)
    summed = (kept + come).astype(jnp.bfloat16).reshape(near, rows, 2 * bands)
    parts = lax.all_to_all(summed, NEAR, 0, 0, tiled=True)
    parts = lax.all_to_all(fold(parts, far), FAR, 0, 0, tiled=True)
    chunk = core * near + lax.axis_index(NEAR)
    mine = weigh(chunk.reshape(1), parts, coupling.reshape(slots, PROJ), near)
    own = lax.all_to_all(mine, NEAR, 0, 0, tiled=True)
    other = lax.ppermute(own, CORE, swap)
    estimate = pl.CostEstimate(
        flops=4 * slots * planes * bands, bytes_accessed=4 * 1024 * 1024, transcendentals=0
    )
    params = pltpu.CompilerParams(vmem_limit_bytes=32 * 1024 * 1024)
    total = pl.pallas_call(
        first_kernel,
        out_shape=jax.ShapeDtypeStruct((2 * bands, planes), jnp.float32),
        in_specs=[vmem] * 3,
        out_specs=vmem,
        cost_estimate=estimate,
        compiler_params=params,
        name="spread_own",
    )(own, real_own, imag_own)
    applied, energy = pl.pallas_call(
        functools.partial(last_kernel, float(slots)),
        out_shape=(
            jax.ShapeDtypeStruct((2 * bands, planes), jnp.bfloat16),
            jax.ShapeDtypeStruct((1, bands), jnp.float32),
        ),
        in_specs=[vmem] * 5,
        out_specs=(vmem, vmem),
        cost_estimate=estimate,
        compiler_params=params,
        name="spread_other",
    )(own, other, real_other, imag_other, total)
    return applied.reshape(2, bands, planes), energy.reshape(bands)


def solution(mesh):
    split = Mesh(
        mesh.devices.reshape(mesh.shape["kpt"], 4, 4, 4, 2), ("kpt", "x", "zh", "zl", "c")
    )
    in_specs = (P(None, GA), P("kpt"), P(None, "kpt", GA), P(), P(), P(), P(), P())
    out_specs = (P(None, "kpt", GA), P("kpt"))
    return jax.shard_map(
        on_device, mesh=split, in_specs=in_specs, out_specs=out_specs, check_vma=False
    )
```

```python
import functools
import math

import jax
import jax.numpy as jnp
import numpy as np
from jax import lax
from jax.experimental import pallas as pl
from jax.experimental.pallas import tpu as pltpu
from jax.sharding import Mesh
from jax.sharding import PartitionSpec as P

PROJ = 8
MGRID = 64
GA = ("x", "z", "c")
NEAR = ("x", "z")
FAR = "z"
CORE = "c"
EXTRA = 8
SMALL = 8 * 1024 * 1024


def groups_of(wide, ring, span=4):
    blocks = ring // span
    turn = [span // 2 if 2 * b >= blocks else 0 for b in range(blocks)]
    place = [[b * span + (q + turn[b]) % span for q in range(span)] for b in range(blocks)]
    near = [[w * ring + z for w in range(wide) for z in place[b]] for b in range(blocks)]
    far = [[place[b][q] for b in range(blocks)] for q in range(span)]
    return near, far


def turn_series(degree=9):
    nodes = 0.125 + 0.125 * np.cos(np.pi * (np.arange(64) + 0.5) / 64)
    root = np.sqrt(nodes)
    fit = np.polynomial.chebyshev.Chebyshev.fit
    poly = np.polynomial.Polynomial
    cosine = fit(nodes, np.cos(2 * np.pi * root), degree, domain=[0, 0.25]).convert(kind=poly)
    sine = fit(nodes, np.sin(2 * np.pi * root) / root, degree, domain=[0, 0.25]).convert(kind=poly)
    return [float(v) for v in cosine.coef], [float(v) for v in sine.coef]


COSINE, SINE = turn_series()


def series(coefficients, y):
    total = jnp.full_like(y, coefficients[-1])
    for value in coefficients[-2::-1]:
        total = total * y + value
    return total


def nearest(x):
    return jnp.floor(x + 0.5)


def build_kernel(
    scaling,
    half_ref,
    kpoint_hbm,
    species_hbm,
    counts_hbm,
    miller_hbm,
    waves_hbm,
    positions_hbm,
    radial_hbm,
    over_ref,
    real_ref,
    imag_ref,
    amp_ref,
    cos_ref,
    sin_ref,
    kpoint_ref,
    species_ref,
    counts_ref,
    miller_ref,
    waves_ref,
    positions_ref,
    radial_ref,
    done,
):
    f32, bf16 = jnp.float32, jnp.bfloat16
    pairs = (
        (miller_hbm, miller_ref),
        (kpoint_hbm, kpoint_ref),
        (radial_hbm, radial_ref),
        (positions_hbm, positions_ref),
        (species_hbm, species_ref),
        (counts_hbm, counts_ref),
        (waves_hbm, waves_ref),
    )
    copies = [pltpu.make_async_copy(a, b, done.at[i]) for i, (a, b) in enumerate(pairs)]
    for copy in copies:
        copy.start()
    terms = radial_ref.shape[1]
    planes = miller_ref.shape[1]
    slots = real_ref.shape[0]
    atoms = slots // PROJ
    kinds = radial_ref.shape[0] // PROJ
    half = half_ref[0]
    for copy in copies[:-1]:
        copy.wait()

    miller = miller_ref[...].astype(f32)
    shifted = [miller[c : c + 1] + kpoint_ref[c] for c in range(3)]
    squared = shifted[0] * shifted[0] + shifted[1] * shifted[1] + shifted[2] * shifted[2]
    order = lax.broadcasted_iota(jnp.int32, (terms, planes), 0)
    widths = jnp.zeros((terms, planes), f32)
    for r in range(terms):
        widths = jnp.where(order == r, 0.001 * 1.5**r, widths)
    basis = jnp.exp(-widths * squared)
    radial = jnp.dot(
        radial_ref[...], basis, precision=lax.Precision.HIGHEST, preferred_element_type=f32
    )
    scale = 1.0 / jnp.sqrt(squared + 1.0)
    row = lax.broadcasted_iota(jnp.int32, (PROJ, planes), 0) % 4
    angular = jnp.where(row == 0, 1.0, jnp.where(row == 1, shifted[0] * scale, 0.0))
    angular = jnp.where(row == 2, shifted[1] * scale, angular)
    angular = jnp.where(row == 3, shifted[2] * scale, angular) * scaling
    for s in range(kinds):
        amp_ref[s * PROJ : (s + 1) * PROJ, :] = radial[s * PROJ : (s + 1) * PROJ] * angular

    places = positions_ref[...].astype(f32)
    third = lax.broadcasted_iota(jnp.int32, (3, 128), 0)
    point = jnp.where(third == 0, kpoint_ref[0], jnp.where(third == 1, kpoint_ref[1], kpoint_ref[2]))
    inner = (((0,), (0,)), ((), ()))
    winding = lax.dot_general(
        places.astype(bf16), miller.astype(bf16), inner, preferred_element_type=f32
    )
    offset = lax.dot_general(
        places, point, inner, precision=lax.Precision.HIGHEST, preferred_element_type=f32
    )
    winding = winding * (1.0 / MGRID)
    offset = offset * (1.0 / MGRID)
    winding = winding - nearest(winding)
    offset = offset - nearest(offset)
    cos_ref[...] = winding + jnp.concatenate([offset] * (planes // 128), 1)

    first = pl.multiple_of(half * atoms, atoms)
    turns = cos_ref[pl.ds(first, atoms), :]
    turns = turns - nearest(turns)
    square = turns * turns
    cosine = series(COSINE, square)
    sine = series(SINE, square) * -turns
    cos_ref[0:atoms, :] = cosine
    sin_ref[...] = sine

    slot = lax.broadcasted_iota(jnp.int32, (PROJ, planes), 0)
    per = 4

    def build(step, carry):
        real, imag = [], []
        for k in range(per):
            at = step * per + k
            kind = species_ref[first + at]
            number = counts_ref[first + at]
            amp = amp_ref[pl.ds(pl.multiple_of(kind * PROJ, PROJ), PROJ), :]
            amp = jnp.where(slot < number, amp, 0.0)
            real.append(amp * cos_ref[pl.ds(at, 1), :])
            imag.append(amp * sin_ref[pl.ds(at, 1), :])
        rows = pl.ds(pl.multiple_of(step * per * PROJ, per * PROJ), per * PROJ)
        real_ref[rows, :] = jnp.concatenate(real, 0).astype(bf16)
        imag_ref[rows, :] = jnp.concatenate(imag, 0).astype(bf16)
        return carry

    lax.fori_loop(0, atoms // per, build, 0)

    copies[-1].wait()
    waves = waves_ref[...]
    bands = waves.shape[0] // 2
    turned = jnp.concatenate([waves[bands:], -waves[:bands]], 0)
    outer = (((1,), (1,)), ((), ()))
    over_ref[...] = lax.dot_general(
        real_ref[...], waves, outer, preferred_element_type=f32
    ) + lax.dot_general(imag_ref[...], turned, outer, preferred_element_type=f32)


def build_half(half, scaling, kpoint, species, counts, miller, waves, positions, radial):
    planes = miller.shape[1]
    atoms = species.shape[0] // 2
    slots = atoms * PROJ
    smem = pl.BlockSpec(memory_space=pltpu.SMEM)
    vmem = pl.BlockSpec(memory_space=pltpu.VMEM)
    hbm = pl.BlockSpec(memory_space=pltpu.HBM)
    shape = jax.ShapeDtypeStruct
    whole = [kpoint, species, counts, miller, waves, positions, radial]
    whole = [pltpu.with_memory_space_constraint(a, pltpu.HBM) for a in whole]
    return pl.pallas_call(
        functools.partial(build_kernel, scaling),
        out_shape=(
            shape((slots, waves.shape[0]), jnp.float32),
            shape((slots, planes), jnp.bfloat16),
            shape((slots, planes), jnp.bfloat16),
        ),
        in_specs=[smem] + [hbm] * 7,
        out_specs=(vmem,) * 3,
        scratch_shapes=[
            pltpu.VMEM((radial.shape[0], planes), jnp.float32),
            pltpu.VMEM((2 * atoms, planes), jnp.float32),
            pltpu.VMEM((atoms, planes), jnp.float32),
            pltpu.SMEM(kpoint.shape, kpoint.dtype),
            pltpu.SMEM(species.shape, species.dtype),
            pltpu.SMEM(counts.shape, counts.dtype),
            pltpu.VMEM(miller.shape, miller.dtype),
            pltpu.VMEM(waves.shape, waves.dtype),
            pltpu.VMEM(positions.shape, positions.dtype),
            pltpu.VMEM(radial.shape, radial.dtype),
            pltpu.SemaphoreType.DMA((7,)),
        ],
        cost_estimate=pl.CostEstimate(
            flops=8 * slots * planes * 128, bytes_accessed=4 * 1024 * 1024, transcendentals=0
        ),
        compiler_params=pltpu.CompilerParams(vmem_limit_bytes=32 * 1024 * 1024),
        name="build",
    )(half, *whole)


def fold_kernel(parts_ref, out_ref):
    total = jnp.sum(parts_ref[...].astype(jnp.float32), axis=0).astype(out_ref.dtype)
    for k in range(out_ref.shape[0]):
        out_ref[k] = total


def fold(parts, copies):
    return pl.pallas_call(
        fold_kernel,
        out_shape=pltpu.VMEM((copies, *parts.shape[1:]), parts.dtype),
        in_specs=[pl.BlockSpec(memory_space=pltpu.VMEM)],
        out_specs=pl.BlockSpec(memory_space=pltpu.VMEM),
        compiler_params=pltpu.CompilerParams(vmem_limit_bytes=SMALL),
        name="fold",
    )(parts)


def weigh_kernel(chunk_ref, parts_ref, coupling_ref, out_ref):
    f32, bf16 = jnp.float32, jnp.bfloat16
    over = jnp.sum(parts_ref[...].astype(f32), axis=0)
    rows, both = over.shape
    bands = both // 2
    matrix = coupling_ref[pl.ds(pl.multiple_of(chunk_ref[0] * rows, rows), rows), :]
    weighted = []
    for k in range(rows // PROJ):
        block = over[k * PROJ : (k + 1) * PROJ]
        part = matrix[k * PROJ : (k + 1) * PROJ]
        total = part[:, 0:1] * block[0:1]
        for j in range(1, PROJ):
            total = total + part[:, j : j + 1] * block[j : j + 1]
        weighted.append(total)
    weighted = jnp.concatenate(weighted, 0)
    energy = jnp.sum(over * weighted, axis=0, keepdims=True)
    energy = energy[:, :bands] + energy[:, bands:]
    high = energy.astype(bf16).astype(f32)
    share = jnp.concatenate([high, energy - high], 1)
    index = lax.broadcasted_iota(jnp.int32, (EXTRA, both), 0)
    share = jnp.where(index == 0, share, 0.0)
    whole = jnp.concatenate([weighted, share], 0).astype(bf16)
    for k in range(out_ref.shape[0]):
        out_ref[k] = whole


def weigh(chunk, parts, coupling, copies):
    rows, both = parts.shape[1:]
    smem = pl.BlockSpec(memory_space=pltpu.SMEM)
    vmem = pl.BlockSpec(memory_space=pltpu.VMEM)
    return pl.pallas_call(
        weigh_kernel,
        out_shape=jax.ShapeDtypeStruct((copies, rows + EXTRA, both), jnp.bfloat16),
        in_specs=[smem, vmem, vmem],
        out_specs=vmem,
        compiler_params=pltpu.CompilerParams(vmem_limit_bytes=SMALL),
        name="weigh",
    )(chunk, parts, coupling)


def spread(table_ref, real_ref, imag_ref):
    copies, rows, both = table_ref.shape
    rows = rows - EXTRA
    bands = both // 2
    table = table_ref[:, 0:rows, :].reshape(copies * rows, both)
    turned = jnp.concatenate([-table[:, bands:], table[:, :bands]], 1)
    inner = (((0,), (0,)), ((), ()))
    return lax.dot_general(
        table, real_ref[...], inner, preferred_element_type=jnp.float32
    ) + lax.dot_general(turned, imag_ref[...], inner, preferred_element_type=jnp.float32)


def share_of(table_ref):
    both = table_ref.shape[2]
    rows = table_ref.shape[1] - EXTRA
    share = jnp.sum(table_ref[:, rows:, :].astype(jnp.float32), axis=(0, 1), keepdims=True)[0]
    return share[:, : both // 2] + share[:, both // 2 :]


def first_kernel(table_ref, real_ref, imag_ref, out_ref):
    out_ref[...] = spread(table_ref, real_ref, imag_ref)


def last_kernel(slots, own_ref, table_ref, real_ref, imag_ref, total_ref, out_ref, energy_ref):
    out_ref[...] = (total_ref[...] + spread(table_ref, real_ref, imag_ref)).astype(out_ref.dtype)
    energy_ref[...] = (share_of(own_ref) + share_of(table_ref)) / slots


def on_device(miller_index, kpoint, waves, species, counts, positions, radial_coef, coupling):
    planes = waves.shape[2]
    bands = waves.shape[1]
    scaling = 1.0 / math.sqrt(planes * lax.axis_size(GA))
    slots = coupling.shape[0] * PROJ
    near_groups, far_groups = groups_of(lax.axis_size("x"), lax.axis_size("z"))
    near, far, span = len(near_groups[0]), len(far_groups[0]), len(far_groups)
    rows = slots // (2 * near)
    along = lax.axis_index("z")
    turn = jnp.where(2 * along >= lax.axis_size("z"), span // 2, 0)
    chunk = lax.axis_index(CORE) * near + lax.axis_index("x") * span + (along + turn) % span
    vmem = pl.BlockSpec(memory_space=pltpu.VMEM)
    core = lax.axis_index(CORE)
    swap = [(0, 1), (1, 0)]
    flat = waves.reshape(2 * bands, planes)
    radial = radial_coef.reshape(-1, radial_coef.shape[2])

    def build(half):
        return build_half(
            half.reshape(1), scaling, kpoint, species, counts, miller_index, flat, positions, radial
        )

    sent, real_other, imag_other = build(1 - core)
    come = lax.ppermute(sent, CORE, swap)
    kept, real_own, imag_own = build(core)
    summed = (kept + come).astype(jnp.bfloat16).reshape(near, rows, 2 * bands)
    exchange = functools.partial(lax.all_to_all, split_axis=0, concat_axis=0, tiled=True)
    parts = exchange(summed, NEAR, axis_index_groups=near_groups)
    parts = exchange(fold(parts, far), FAR, axis_index_groups=far_groups)
    mine = weigh(chunk.reshape(1), parts, coupling.reshape(slots, PROJ), near)
    own = exchange(mine, NEAR, axis_index_groups=near_groups)
    other = lax.ppermute(own, CORE, swap)
    estimate = pl.CostEstimate(
        flops=4 * slots * planes * bands, bytes_accessed=4 * 1024 * 1024, transcendentals=0
    )
    params = pltpu.CompilerParams(vmem_limit_bytes=32 * 1024 * 1024)
    total = pl.pallas_call(
        first_kernel,
        out_shape=jax.ShapeDtypeStruct((2 * bands, planes), jnp.float32),
        in_specs=[vmem] * 3,
        out_specs=vmem,
        cost_estimate=estimate,
        compiler_params=params,
        name="spread_own",
    )(own, real_own, imag_own)
    applied, energy = pl.pallas_call(
        functools.partial(last_kernel, float(slots)),
        out_shape=(
            jax.ShapeDtypeStruct((2 * bands, planes), jnp.bfloat16),
            jax.ShapeDtypeStruct((1, bands), jnp.float32),
        ),
        in_specs=[vmem] * 5,
        out_specs=(vmem, vmem),
        cost_estimate=estimate,
        compiler_params=params,
        name="spread_other",
    )(own, other, real_other, imag_other, total)
    return applied.reshape(2, bands, planes), energy.reshape(bands)


def solution(mesh):
    split = Mesh(
        mesh.devices.reshape(mesh.shape["kpt"], 4, 16, 2), ("kpt", *GA)
    )
    in_specs = (P(None, GA), P("kpt"), P(None, "kpt", GA), P(), P(), P(), P(), P())
    out_specs = (P(None, "kpt", GA), P("kpt"))
    return jax.shard_map(
        on_device, mesh=split, in_specs=in_specs, out_specs=out_specs, check_vma=False
    )
```

```python
import functools
import math

import jax
import jax.numpy as jnp
import numpy as np
from jax import lax
from jax.experimental import pallas as pl
from jax.experimental.pallas import tpu as pltpu
from jax.sharding import Mesh
from jax.sharding import PartitionSpec as P

PROJ = 8
MGRID = 64
GA = ("x", "z", "c")
NEAR = ("x", "z")
FAR = "z"
CORE = "c"
EXTRA = 8
SMALL = 8 * 1024 * 1024


def groups_of(wide, ring, span=4):
    blocks = ring // span
    inner = [*range(1, span - 1), 0, span - 1]
    turn = [span // 2 if 2 * b >= blocks else 0 for b in range(blocks)]
    place = [[b * span + (q + turn[b]) % span for q in inner] for b in range(blocks)]
    near = [[w * ring + z for w in range(wide) for z in place[b]] for b in range(blocks)]
    late = [*range(blocks // 2, blocks), *range(blocks // 2)]
    far = [[place[b][q] for b in late] for q in range(span)]
    return near, far


def turn_series(degree=9):
    nodes = 0.125 + 0.125 * np.cos(np.pi * (np.arange(64) + 0.5) / 64)
    root = np.sqrt(nodes)
    fit = np.polynomial.chebyshev.Chebyshev.fit
    poly = np.polynomial.Polynomial
    cosine = fit(nodes, np.cos(2 * np.pi * root), degree, domain=[0, 0.25]).convert(kind=poly)
    sine = fit(nodes, np.sin(2 * np.pi * root) / root, degree, domain=[0, 0.25]).convert(kind=poly)
    return [float(v) for v in cosine.coef], [float(v) for v in sine.coef]


COSINE, SINE = turn_series()


def series(coefficients, y):
    total = jnp.full_like(y, coefficients[-1])
    for value in coefficients[-2::-1]:
        total = total * y + value
    return total


def nearest(x):
    return jnp.floor(x + 0.5)


def fill(first, amp_ref, cos_ref, sin_ref, species_ref, counts_ref, real_ref, imag_ref, per=4):
    atoms, planes = sin_ref.shape
    slot = lax.broadcasted_iota(jnp.int32, (PROJ, planes), 0)

    def step(index, carry):
        real, imag = [], []
        for k in range(per):
            at = index * per + k
            kind = species_ref[first + at]
            number = counts_ref[first + at]
            amp = amp_ref[pl.ds(pl.multiple_of(kind * PROJ, PROJ), PROJ), :]
            amp = jnp.where(slot < number, amp, 0.0)
            real.append(amp * cos_ref[pl.ds(at, 1), :])
            imag.append(amp * sin_ref[pl.ds(at, 1), :])
        rows = pl.ds(pl.multiple_of(index * per * PROJ, per * PROJ), per * PROJ)
        real_ref[rows, :] = jnp.concatenate(real, 0).astype(jnp.bfloat16)
        imag_ref[rows, :] = jnp.concatenate(imag, 0).astype(jnp.bfloat16)
        return carry

    lax.fori_loop(0, atoms // per, step, 0)


def wave_pair(turns):
    turns = turns - nearest(turns)
    square = turns * turns
    return series(COSINE, square), series(SINE, square) * -turns


def overlap(real_ref, imag_ref, waves):
    bands = waves.shape[0] // 2
    turned = jnp.concatenate([waves[bands:], -waves[:bands]], 0)
    outer = (((1,), (1,)), ((), ()))
    return lax.dot_general(
        real_ref[...], waves, outer, preferred_element_type=jnp.float32
    ) + lax.dot_general(imag_ref[...], turned, outer, preferred_element_type=jnp.float32)


def send_kernel(
    scaling,
    half_ref,
    kpoint_hbm,
    species_hbm,
    counts_hbm,
    miller_hbm,
    waves_hbm,
    positions_hbm,
    radial_hbm,
    over_ref,
    real_ref,
    imag_ref,
    amp_ref,
    rest_ref,
    waves_ref,
    species_out,
    counts_out,
    all_ref,
    cos_ref,
    sin_ref,
    kpoint_ref,
    species_ref,
    counts_ref,
    miller_ref,
    positions_ref,
    radial_ref,
    done,
):
    f32, bf16 = jnp.float32, jnp.bfloat16
    pairs = (
        (miller_hbm, miller_ref),
        (kpoint_hbm, kpoint_ref),
        (radial_hbm, radial_ref),
        (positions_hbm, positions_ref),
        (species_hbm, species_ref),
        (counts_hbm, counts_ref),
        (species_hbm, species_out),
        (counts_hbm, counts_out),
        (waves_hbm, waves_ref),
    )
    copies = [pltpu.make_async_copy(a, b, done.at[i]) for i, (a, b) in enumerate(pairs)]
    for copy in copies:
        copy.start()
    terms = radial_ref.shape[1]
    planes = miller_ref.shape[1]
    atoms = sin_ref.shape[0]
    kinds = radial_ref.shape[0] // PROJ
    half = half_ref[0]
    for copy in copies[:-3]:
        copy.wait()

    miller = miller_ref[...].astype(f32)
    shifted = [miller[c : c + 1] + kpoint_ref[c] for c in range(3)]
    squared = shifted[0] * shifted[0] + shifted[1] * shifted[1] + shifted[2] * shifted[2]
    order = lax.broadcasted_iota(jnp.int32, (terms, planes), 0)
    widths = jnp.zeros((terms, planes), f32)
    for r in range(terms):
        widths = jnp.where(order == r, 0.001 * 1.5**r, widths)
    basis = jnp.exp(-widths * squared)
    radial = jnp.dot(
        radial_ref[...], basis, precision=lax.Precision.HIGHEST, preferred_element_type=f32
    )
    scale = 1.0 / jnp.sqrt(squared + 1.0)
    row = lax.broadcasted_iota(jnp.int32, (PROJ, planes), 0) % 4
    angular = jnp.where(row == 0, 1.0, jnp.where(row == 1, shifted[0] * scale, 0.0))
    angular = jnp.where(row == 2, shifted[1] * scale, angular)
    angular = jnp.where(row == 3, shifted[2] * scale, angular) * scaling
    for s in range(kinds):
        amp_ref[s * PROJ : (s + 1) * PROJ, :] = radial[s * PROJ : (s + 1) * PROJ] * angular

    places = positions_ref[...].astype(f32)
    third = lax.broadcasted_iota(jnp.int32, (3, 128), 0)
    point = jnp.where(third == 0, kpoint_ref[0], jnp.where(third == 1, kpoint_ref[1], kpoint_ref[2]))
    inner = (((0,), (0,)), ((), ()))
    winding = lax.dot_general(
        places.astype(bf16), miller.astype(bf16), inner, preferred_element_type=f32
    )
    offset = lax.dot_general(
        places, point, inner, precision=lax.Precision.HIGHEST, preferred_element_type=f32
    )
    winding = winding * (1.0 / MGRID)
    offset = offset * (1.0 / MGRID)
    winding = winding - nearest(winding)
    offset = offset - nearest(offset)
    all_ref[...] = winding + jnp.concatenate([offset] * (planes // 128), 1)
    first = pl.multiple_of(half * atoms, atoms)
    other = pl.multiple_of((1 - half) * atoms, atoms)
    rest_ref[...] = all_ref[pl.ds(other, atoms), :]
    cosine, sine = wave_pair(all_ref[pl.ds(first, atoms), :])
    cos_ref[...] = cosine
    sin_ref[...] = sine
    fill(first, amp_ref, cos_ref, sin_ref, species_ref, counts_ref, real_ref, imag_ref)
    for copy in copies[-3:]:
        copy.wait()
    over_ref[...] = overlap(real_ref, imag_ref, waves_ref[...])


def keep_kernel(
    half_ref,
    species_vmem,
    counts_vmem,
    amp_ref,
    turns_ref,
    waves_ref,
    over_ref,
    real_ref,
    imag_ref,
    cos_ref,
    sin_ref,
    species_ref,
    counts_ref,
    done,
):
    copies = [
        pltpu.make_async_copy(species_vmem, species_ref, done.at[0]),
        pltpu.make_async_copy(counts_vmem, counts_ref, done.at[1]),
    ]
    for copy in copies:
        copy.start()
    cosine, sine = wave_pair(turns_ref[...])
    cos_ref[...] = cosine
    sin_ref[...] = sine
    for copy in copies:
        copy.wait()
    first = half_ref[0] * cos_ref.shape[0]
    fill(first, amp_ref, cos_ref, sin_ref, species_ref, counts_ref, real_ref, imag_ref)
    over_ref[...] = overlap(real_ref, imag_ref, waves_ref[...])


def build_both(core, scaling, kpoint, species, counts, miller, waves, positions, radial):
    planes = miller.shape[1]
    atoms = species.shape[0] // 2
    slots = atoms * PROJ
    smem = pl.BlockSpec(memory_space=pltpu.SMEM)
    vmem = pl.BlockSpec(memory_space=pltpu.VMEM)
    hbm = pl.BlockSpec(memory_space=pltpu.HBM)
    shape = jax.ShapeDtypeStruct
    whole = [kpoint, species, counts, miller, waves, positions, radial]
    whole = [pltpu.with_memory_space_constraint(a, pltpu.HBM) for a in whole]
    results = (
        shape((slots, waves.shape[0]), jnp.float32),
        shape((slots, planes), jnp.bfloat16),
        shape((slots, planes), jnp.bfloat16),
    )
    waving = [pltpu.VMEM((atoms, planes), jnp.float32)] * 2
    tables = [pltpu.SMEM(species.shape, species.dtype), pltpu.SMEM(counts.shape, counts.dtype)]
    estimate = pl.CostEstimate(
        flops=4 * slots * planes * waves.shape[0], bytes_accessed=2**22, transcendentals=0
    )
    params = pltpu.CompilerParams(vmem_limit_bytes=32 * 1024 * 1024)
    *sent, amp, turns, held, kinds, numbers = pl.pallas_call(
        functools.partial(send_kernel, scaling),
        out_shape=(
            *results,
            shape((radial.shape[0], planes), jnp.float32),
            shape((atoms, planes), jnp.float32),
            shape(waves.shape, waves.dtype),
            shape(species.shape, species.dtype),
            shape(counts.shape, counts.dtype),
        ),
        in_specs=[smem] + [hbm] * 7,
        out_specs=(vmem,) * 8,
        scratch_shapes=[
            pltpu.VMEM((2 * atoms, planes), jnp.float32),
            *waving,
            pltpu.SMEM(kpoint.shape, kpoint.dtype),
            *tables,
            pltpu.VMEM(miller.shape, miller.dtype),
            pltpu.VMEM(positions.shape, positions.dtype),
            pltpu.VMEM(radial.shape, radial.dtype),
            pltpu.SemaphoreType.DMA((9,)),
        ],
        cost_estimate=estimate,
        compiler_params=params,
        name="build_send",
    )((1 - core).reshape(1), *whole)
    kept = pl.pallas_call(
        keep_kernel,
        out_shape=results,
        in_specs=[smem] + [vmem] * 5,
        out_specs=(vmem,) * 3,
        scratch_shapes=[*waving, *tables, pltpu.SemaphoreType.DMA((2,))],
        cost_estimate=estimate,
        compiler_params=params,
        name="build_keep",
    )(core.reshape(1), kinds, numbers, amp, turns, held)
    return sent, kept


def fold_kernel(parts_ref, out_ref):
    total = jnp.sum(parts_ref[...].astype(jnp.float32), axis=0).astype(out_ref.dtype)
    for k in range(out_ref.shape[0]):
        out_ref[k] = total


def fold(parts, copies):
    return pl.pallas_call(
        fold_kernel,
        out_shape=pltpu.VMEM((copies, *parts.shape[1:]), parts.dtype),
        in_specs=[pl.BlockSpec(memory_space=pltpu.VMEM)],
        out_specs=pl.BlockSpec(memory_space=pltpu.VMEM),
        compiler_params=pltpu.CompilerParams(vmem_limit_bytes=SMALL),
        name="fold",
    )(parts)


def weigh_kernel(chunk_ref, parts_ref, coupling_ref, out_ref):
    f32, bf16 = jnp.float32, jnp.bfloat16
    over = jnp.sum(parts_ref[...].astype(f32), axis=0)
    rows, both = over.shape
    bands = both // 2
    matrix = coupling_ref[pl.ds(pl.multiple_of(chunk_ref[0] * rows, rows), rows), :]
    weighted = []
    for k in range(rows // PROJ):
        block = over[k * PROJ : (k + 1) * PROJ]
        part = matrix[k * PROJ : (k + 1) * PROJ]
        total = part[:, 0:1] * block[0:1]
        for j in range(1, PROJ):
            total = total + part[:, j : j + 1] * block[j : j + 1]
        weighted.append(total)
    weighted = jnp.concatenate(weighted, 0)
    energy = jnp.sum(over * weighted, axis=0, keepdims=True)
    energy = energy[:, :bands] + energy[:, bands:]
    high = energy.astype(bf16).astype(f32)
    index = lax.broadcasted_iota(jnp.int32, (EXTRA, bands), 0)
    share = jnp.where(index == 0, high, jnp.where(index == 1, energy - high, 0.0))
    whole = jnp.concatenate([weighted[:, :bands], weighted[:, bands:], share], 0).astype(bf16)
    for k in range(out_ref.shape[0]):
        out_ref[k] = whole


def weigh(chunk, parts, coupling, copies):
    rows, both = parts.shape[1:]
    smem = pl.BlockSpec(memory_space=pltpu.SMEM)
    vmem = pl.BlockSpec(memory_space=pltpu.VMEM)
    return pl.pallas_call(
        weigh_kernel,
        out_shape=jax.ShapeDtypeStruct((copies, 2 * rows + EXTRA, both // 2), jnp.bfloat16),
        in_specs=[smem, vmem, vmem],
        out_specs=vmem,
        compiler_params=pltpu.CompilerParams(vmem_limit_bytes=SMALL),
        name="weigh",
    )(chunk, parts, coupling)


def spread(table_ref, real_ref, imag_ref):
    copies, rows, bands = table_ref.shape
    rows = (rows - EXTRA) // 2
    real = table_ref[:, 0:rows, :].reshape(copies * rows, bands)
    imag = table_ref[:, rows : 2 * rows, :].reshape(copies * rows, bands)
    table = jnp.concatenate([real, imag], 1)
    turned = jnp.concatenate([-imag, real], 1)
    inner = (((0,), (0,)), ((), ()))
    return lax.dot_general(
        table, real_ref[...], inner, preferred_element_type=jnp.float32
    ) + lax.dot_general(turned, imag_ref[...], inner, preferred_element_type=jnp.float32)


def share_of(table_ref):
    rows = table_ref.shape[1] - EXTRA
    return jnp.sum(table_ref[:, rows:, :].astype(jnp.float32), axis=(0, 1), keepdims=True)[0]


def first_kernel(table_ref, real_ref, imag_ref, out_ref):
    out_ref[...] = spread(table_ref, real_ref, imag_ref)


def last_kernel(slots, own_ref, table_ref, real_ref, imag_ref, total_ref, out_ref, energy_ref):
    out_ref[...] = (total_ref[...] + spread(table_ref, real_ref, imag_ref)).astype(out_ref.dtype)
    energy_ref[...] = (share_of(own_ref) + share_of(table_ref)) / slots


def on_device(miller_index, kpoint, waves, species, counts, positions, radial_coef, coupling):
    planes = waves.shape[2]
    bands = waves.shape[1]
    scaling = 1.0 / math.sqrt(planes * lax.axis_size(GA))
    slots = coupling.shape[0] * PROJ
    near_groups, far_groups = groups_of(lax.axis_size("x"), lax.axis_size("z"))
    near, far = len(near_groups[0]), len(far_groups[0])
    rows = slots // (2 * near)
    rank = {z: i for group in near_groups for i, z in enumerate(group)}
    rank = jnp.array([rank[i] for i in range(len(rank))], jnp.int32)
    core = lax.axis_index(CORE)
    chunk = core * near + rank[lax.axis_index(NEAR)]
    vmem = pl.BlockSpec(memory_space=pltpu.VMEM)
    swap = [(0, 1), (1, 0)]
    flat = waves.reshape(2 * bands, planes)
    radial = radial_coef.reshape(-1, radial_coef.shape[2])
    sent, kept = build_both(
        core, scaling, kpoint, species, counts, miller_index, flat, positions, radial
    )
    come = lax.ppermute(sent[0], CORE, swap)
    summed = (kept[0] + come).astype(jnp.bfloat16).reshape(near, rows, 2 * bands)
    exchange = functools.partial(lax.all_to_all, split_axis=0, concat_axis=0, tiled=True)
    parts = exchange(summed, NEAR, axis_index_groups=near_groups)
    parts = exchange(fold(parts, far), FAR, axis_index_groups=far_groups)
    mine = weigh(chunk.reshape(1), parts, coupling.reshape(slots, PROJ), near)
    own = exchange(mine, NEAR, axis_index_groups=near_groups)
    other = lax.ppermute(own, CORE, swap)
    estimate = pl.CostEstimate(
        flops=4 * slots * planes * bands, bytes_accessed=4 * 1024 * 1024, transcendentals=0
    )
    params = pltpu.CompilerParams(vmem_limit_bytes=32 * 1024 * 1024)
    total = pl.pallas_call(
        first_kernel,
        out_shape=jax.ShapeDtypeStruct((2 * bands, planes), jnp.float32),
        in_specs=[vmem] * 3,
        out_specs=vmem,
        cost_estimate=estimate,
        compiler_params=params,
        name="spread_own",
    )(own, *kept[1:])
    applied, energy = pl.pallas_call(
        functools.partial(last_kernel, float(slots)),
        out_shape=(
            jax.ShapeDtypeStruct((2 * bands, planes), jnp.bfloat16),
            jax.ShapeDtypeStruct((1, bands), jnp.float32),
        ),
        in_specs=[vmem] * 5,
        out_specs=(vmem, vmem),
        cost_estimate=estimate,
        compiler_params=params,
        name="spread_other",
    )(own, other, *sent[1:3], total)
    return applied.reshape(2, bands, planes), energy.reshape(bands)


def solution(mesh):
    split = Mesh(
        mesh.devices.reshape(mesh.shape["kpt"], 4, 16, 2), ("kpt", *GA)
    )
    in_specs = (P(None, GA), P("kpt"), P(None, "kpt", GA), P(), P(), P(), P(), P())
    out_specs = (P(None, "kpt", GA), P("kpt"))
    return jax.shard_map(
        on_device, mesh=split, in_specs=in_specs, out_specs=out_specs, check_vma=False
    )
```

```python
import functools
import math

import jax
import jax.numpy as jnp
import numpy as np
from jax import lax
from jax.experimental import pallas as pl
from jax.experimental.pallas import tpu as pltpu
from jax.sharding import Mesh
from jax.sharding import PartitionSpec as P

PROJ = 8
MGRID = 64
GA = ("x", "z", "c")
NEAR = ("x", "z")
FAR = "z"
CORE = "c"
EXTRA = 8
SMALL = 8 * 1024 * 1024


def groups_of(wide, ring, span=4):
    blocks = ring // span
    inner = [*range(1, span - 1), 0, span - 1]
    turn = [span // 2 if 2 * b >= blocks else 0 for b in range(blocks)]
    place = [[b * span + (q + turn[b]) % span for q in inner] for b in range(blocks)]
    near = [[w * ring + z for w in range(wide) for z in place[b]] for b in range(blocks)]
    late = [*range(blocks // 2, blocks), *range(blocks // 2)]
    far = [[place[b][q] for b in late] for q in range(span)]
    return near, far


def rank_along(z, ring, span=4):
    q = lax.rem(z + jnp.where(2 * z >= ring, span // 2, 0), span)
    return jnp.where(q == 0, span - 2, jnp.where(q == span - 1, span - 1, q - 1))


def turn_series(degree=9):
    nodes = 0.125 + 0.125 * np.cos(np.pi * (np.arange(64) + 0.5) / 64)
    root = np.sqrt(nodes)
    fit = np.polynomial.chebyshev.Chebyshev.fit
    poly = np.polynomial.Polynomial
    cosine = fit(nodes, np.cos(2 * np.pi * root), degree, domain=[0, 0.25]).convert(kind=poly)
    sine = fit(nodes, np.sin(2 * np.pi * root) / root, degree, domain=[0, 0.25]).convert(kind=poly)
    return [float(v) for v in cosine.coef], [float(v) for v in sine.coef]


COSINE, SINE = turn_series()


def series(coefficients, y):
    total = jnp.full_like(y, coefficients[-1])
    for value in coefficients[-2::-1]:
        total = total * y + value
    return total


def nearest(x):
    return jnp.floor(x + 0.5)


def fill(first, amp_ref, cos_ref, sin_ref, species_ref, counts_ref, real_ref, imag_ref, per=4):
    atoms, planes = sin_ref.shape
    slot = lax.broadcasted_iota(jnp.int32, (PROJ, planes), 0)

    def step(index, carry):
        real, imag = [], []
        for k in range(per):
            at = index * per + k
            kind = species_ref[first + at]
            number = counts_ref[first + at]
            amp = amp_ref[pl.ds(pl.multiple_of(kind * PROJ, PROJ), PROJ), :]
            amp = jnp.where(slot < number, amp, 0.0)
            real.append(amp * cos_ref[pl.ds(at, 1), :])
            imag.append(amp * sin_ref[pl.ds(at, 1), :])
        rows = pl.ds(pl.multiple_of(index * per * PROJ, per * PROJ), per * PROJ)
        real_ref[rows, :] = jnp.concatenate(real, 0).astype(jnp.bfloat16)
        imag_ref[rows, :] = jnp.concatenate(imag, 0).astype(jnp.bfloat16)
        return carry

    lax.fori_loop(0, atoms // per, step, 0)


def wave_pair(turns):
    turns = turns - nearest(turns)
    square = turns * turns
    return series(COSINE, square), series(SINE, square) * -turns


def overlap(real_ref, imag_ref, waves):
    bands = waves.shape[0] // 2
    turned = jnp.concatenate([waves[bands:], -waves[:bands]], 0)
    outer = (((1,), (1,)), ((), ()))
    return lax.dot_general(
        real_ref[...], waves, outer, preferred_element_type=jnp.float32
    ) + lax.dot_general(imag_ref[...], turned, outer, preferred_element_type=jnp.float32)


def send_kernel(
    scaling,
    chunk_atoms,
    half_ref,
    chunk_ref,
    kpoint_hbm,
    species_hbm,
    counts_hbm,
    miller_hbm,
    waves_hbm,
    positions_hbm,
    radial_hbm,
    coupling_hbm,
    over_ref,
    real_ref,
    imag_ref,
    amp_ref,
    rest_ref,
    waves_ref,
    species_out,
    counts_out,
    matrix_ref,
    all_ref,
    cos_ref,
    sin_ref,
    kpoint_ref,
    species_ref,
    counts_ref,
    miller_ref,
    positions_ref,
    radial_ref,
    coupling_ref,
    done,
):
    f32, bf16 = jnp.float32, jnp.bfloat16
    pairs = (
        (miller_hbm, miller_ref),
        (kpoint_hbm, kpoint_ref),
        (radial_hbm, radial_ref),
        (positions_hbm, positions_ref),
        (species_hbm, species_ref),
        (counts_hbm, counts_ref),
        (species_hbm, species_out),
        (counts_hbm, counts_out),
        (coupling_hbm, coupling_ref),
        (waves_hbm, waves_ref),
    )
    copies = [pltpu.make_async_copy(a, b, done.at[i]) for i, (a, b) in enumerate(pairs)]
    for copy in copies:
        copy.start()
    terms = radial_ref.shape[1]
    planes = miller_ref.shape[1]
    atoms = sin_ref.shape[0]
    kinds = radial_ref.shape[0] // PROJ
    half = half_ref[0]
    for copy in copies[:-4]:
        copy.wait()

    miller = miller_ref[...].astype(f32)
    shifted = [miller[c : c + 1] + kpoint_ref[c] for c in range(3)]
    squared = shifted[0] * shifted[0] + shifted[1] * shifted[1] + shifted[2] * shifted[2]
    order = lax.broadcasted_iota(jnp.int32, (terms, planes), 0)
    widths = jnp.zeros((terms, planes), f32)
    for r in range(terms):
        widths = jnp.where(order == r, 0.001 * 1.5**r, widths)
    basis = jnp.exp(-widths * squared)
    radial = jnp.dot(
        radial_ref[...], basis, precision=lax.Precision.HIGHEST, preferred_element_type=f32
    )
    scale = 1.0 / jnp.sqrt(squared + 1.0)
    row = lax.broadcasted_iota(jnp.int32, (PROJ, planes), 0) % 4
    angular = jnp.where(row == 0, 1.0, jnp.where(row == 1, shifted[0] * scale, 0.0))
    angular = jnp.where(row == 2, shifted[1] * scale, angular)
    angular = jnp.where(row == 3, shifted[2] * scale, angular) * scaling
    for s in range(kinds):
        amp_ref[s * PROJ : (s + 1) * PROJ, :] = radial[s * PROJ : (s + 1) * PROJ] * angular

    places = positions_ref[...].astype(f32)
    third = lax.broadcasted_iota(jnp.int32, (3, 128), 0)
    point = jnp.where(third == 0, kpoint_ref[0], jnp.where(third == 1, kpoint_ref[1], kpoint_ref[2]))
    inner = (((0,), (0,)), ((), ()))
    winding = lax.dot_general(
        places.astype(bf16), miller.astype(bf16), inner, preferred_element_type=f32
    )
    offset = lax.dot_general(
        places, point, inner, precision=lax.Precision.HIGHEST, preferred_element_type=f32
    )
    winding = winding * (1.0 / MGRID)
    offset = offset * (1.0 / MGRID)
    winding = winding - nearest(winding)
    offset = offset - nearest(offset)
    all_ref[...] = winding + jnp.concatenate([offset] * (planes // 128), 1)
    first = pl.multiple_of(half * atoms, atoms)
    other = pl.multiple_of((1 - half) * atoms, atoms)
    rest_ref[...] = all_ref[pl.ds(other, atoms), :]
    cosine, sine = wave_pair(all_ref[pl.ds(first, atoms), :])
    cos_ref[...] = cosine
    sin_ref[...] = sine
    fill(first, amp_ref, cos_ref, sin_ref, species_ref, counts_ref, real_ref, imag_ref)
    for copy in copies[-4:]:
        copy.wait()
    lanes = coupling_ref.shape[1]
    matrix_ref[...] = pltpu.roll(coupling_ref[...], lanes - chunk_ref[0] * chunk_atoms, 1)
    over_ref[...] = overlap(real_ref, imag_ref, waves_ref[...])


def keep_kernel(
    half_ref,
    species_vmem,
    counts_vmem,
    amp_ref,
    turns_ref,
    waves_ref,
    over_ref,
    real_ref,
    imag_ref,
    cos_ref,
    sin_ref,
    species_ref,
    counts_ref,
    done,
):
    copies = [
        pltpu.make_async_copy(species_vmem, species_ref, done.at[0]),
        pltpu.make_async_copy(counts_vmem, counts_ref, done.at[1]),
    ]
    for copy in copies:
        copy.start()
    cosine, sine = wave_pair(turns_ref[...])
    cos_ref[...] = cosine
    sin_ref[...] = sine
    for copy in copies:
        copy.wait()
    first = half_ref[0] * cos_ref.shape[0]
    fill(first, amp_ref, cos_ref, sin_ref, species_ref, counts_ref, real_ref, imag_ref)
    over_ref[...] = overlap(real_ref, imag_ref, waves_ref[...])


def build_both(core, chunk, chunk_atoms, scaling, kpoint, species, counts, miller, waves, positions, radial, coupling):
    planes = miller.shape[1]
    atoms = species.shape[0] // 2
    slots = atoms * PROJ
    smem = pl.BlockSpec(memory_space=pltpu.SMEM)
    vmem = pl.BlockSpec(memory_space=pltpu.VMEM)
    hbm = pl.BlockSpec(memory_space=pltpu.HBM)
    shape = jax.ShapeDtypeStruct
    whole = [kpoint, species, counts, miller, waves, positions, radial, coupling]
    whole = [pltpu.with_memory_space_constraint(a, pltpu.HBM) for a in whole]
    results = (
        shape((slots, waves.shape[0]), jnp.float32),
        shape((slots, planes), jnp.bfloat16),
        shape((slots, planes), jnp.bfloat16),
    )
    waving = [pltpu.VMEM((atoms, planes), jnp.float32)] * 2
    tables = [pltpu.SMEM(species.shape, species.dtype), pltpu.SMEM(counts.shape, counts.dtype)]
    estimate = pl.CostEstimate(
        flops=4 * slots * planes * waves.shape[0], bytes_accessed=2**22, transcendentals=0
    )
    params = pltpu.CompilerParams(vmem_limit_bytes=32 * 1024 * 1024)
    *sent, amp, turns, held, kinds, numbers, matrix = pl.pallas_call(
        functools.partial(send_kernel, scaling, chunk_atoms),
        out_shape=(
            *results,
            shape((radial.shape[0], planes), jnp.float32),
            shape((atoms, planes), jnp.float32),
            shape(waves.shape, waves.dtype),
            shape(species.shape, species.dtype),
            shape(counts.shape, counts.dtype),
            shape(coupling.shape, coupling.dtype),
        ),
        in_specs=[smem] * 2 + [hbm] * 8,
        out_specs=(vmem,) * 9,
        scratch_shapes=[
            pltpu.VMEM((2 * atoms, planes), jnp.float32),
            *waving,
            pltpu.SMEM(kpoint.shape, kpoint.dtype),
            *tables,
            pltpu.VMEM(miller.shape, miller.dtype),
            pltpu.VMEM(positions.shape, positions.dtype),
            pltpu.VMEM(radial.shape, radial.dtype),
            pltpu.VMEM(coupling.shape, coupling.dtype),
            pltpu.SemaphoreType.DMA((10,)),
        ],
        cost_estimate=estimate,
        compiler_params=params,
        name="build_send",
    )((1 - core).reshape(1), chunk.reshape(1), *whole)
    kept = pl.pallas_call(
        keep_kernel,
        out_shape=results,
        in_specs=[smem] + [vmem] * 5,
        out_specs=(vmem,) * 3,
        scratch_shapes=[*waving, *tables, pltpu.SemaphoreType.DMA((2,))],
        cost_estimate=estimate,
        compiler_params=params,
        name="build_keep",
    )(core.reshape(1), kinds, numbers, amp, turns, held)
    return sent, kept, matrix


def fold_kernel(parts_ref, out_ref):
    total = jnp.sum(parts_ref[...].astype(jnp.float32), axis=0).astype(out_ref.dtype)
    for k in range(out_ref.shape[0]):
        out_ref[k] = total


def fold(parts, copies):
    return pl.pallas_call(
        fold_kernel,
        out_shape=pltpu.VMEM((copies, *parts.shape[1:]), parts.dtype),
        in_specs=[pl.BlockSpec(memory_space=pltpu.VMEM)],
        out_specs=pl.BlockSpec(memory_space=pltpu.VMEM),
        compiler_params=pltpu.CompilerParams(vmem_limit_bytes=SMALL),
        name="fold",
    )(parts)


def weigh_kernel(parts_ref, matrix_ref, out_ref):
    f32, bf16 = jnp.float32, jnp.bfloat16
    over = jnp.sum(parts_ref[...].astype(f32), axis=0)
    rows, both = over.shape
    bands = both // 2
    weighted = []
    for k in range(rows // PROJ):
        block = over[k * PROJ : (k + 1) * PROJ]
        total = 0.0
        for j in range(PROJ):
            total = total + matrix_ref[j * PROJ : (j + 1) * PROJ, k : k + 1] * block[j : j + 1]
        weighted.append(total)
    weighted = jnp.concatenate(weighted, 0)
    energy = jnp.sum(over * weighted, axis=0, keepdims=True)
    energy = energy[:, :bands] + energy[:, bands:]
    high = energy.astype(bf16).astype(f32)
    index = lax.broadcasted_iota(jnp.int32, (EXTRA, bands), 0)
    share = jnp.where(index == 0, high, jnp.where(index == 1, energy - high, 0.0))
    whole = jnp.concatenate([weighted[:, :bands], weighted[:, bands:], share], 0).astype(bf16)
    for k in range(out_ref.shape[0]):
        out_ref[k] = whole


def weigh(parts, matrix, copies):
    rows, both = parts.shape[1:]
    vmem = pl.BlockSpec(memory_space=pltpu.VMEM)
    return pl.pallas_call(
        weigh_kernel,
        out_shape=jax.ShapeDtypeStruct((copies, 2 * rows + EXTRA, both // 2), jnp.bfloat16),
        in_specs=[vmem, vmem],
        out_specs=vmem,
        compiler_params=pltpu.CompilerParams(vmem_limit_bytes=SMALL),
        name="weigh",
    )(parts, matrix)


def spread(table_ref, real_ref, imag_ref):
    copies, rows, bands = table_ref.shape
    rows = (rows - EXTRA) // 2
    real = table_ref[:, 0:rows, :].reshape(copies * rows, bands)
    imag = table_ref[:, rows : 2 * rows, :].reshape(copies * rows, bands)
    table = jnp.concatenate([real, imag], 1)
    turned = jnp.concatenate([-imag, real], 1)
    inner = (((0,), (0,)), ((), ()))
    return lax.dot_general(
        table, real_ref[...], inner, preferred_element_type=jnp.float32
    ) + lax.dot_general(turned, imag_ref[...], inner, preferred_element_type=jnp.float32)


def share_of(table_ref):
    rows = table_ref.shape[1] - EXTRA
    return jnp.sum(table_ref[:, rows:, :].astype(jnp.float32), axis=(0, 1), keepdims=True)[0]


def first_kernel(table_ref, real_ref, imag_ref, out_ref):
    out_ref[...] = spread(table_ref, real_ref, imag_ref)


def last_kernel(slots, own_ref, table_ref, real_ref, imag_ref, total_ref, out_ref, energy_ref):
    out_ref[...] = (total_ref[...] + spread(table_ref, real_ref, imag_ref)).astype(out_ref.dtype)
    energy_ref[...] = (share_of(own_ref) + share_of(table_ref)) / slots


def on_device(miller_index, kpoint, waves, species, counts, positions, radial_coef, coupling):
    planes = waves.shape[2]
    bands = waves.shape[1]
    scaling = 1.0 / math.sqrt(planes * lax.axis_size(GA))
    slots = coupling.shape[0] * PROJ
    near_groups, far_groups = groups_of(lax.axis_size("x"), lax.axis_size("z"))
    near, far = len(near_groups[0]), len(far_groups[0])
    rows = slots // (2 * near)
    core = lax.axis_index(CORE)
    rank = rank_along(lax.axis_index("z"), lax.axis_size("z"))
    chunk = core * near + lax.axis_index("x") * len(far_groups) + rank
    vmem = pl.BlockSpec(memory_space=pltpu.VMEM)
    swap = [(0, 1), (1, 0)]
    flat = waves.reshape(2 * bands, planes)
    radial = radial_coef.reshape(-1, radial_coef.shape[2])
    by_atom = jnp.transpose(coupling, (1, 2, 0)).reshape(PROJ * PROJ, -1)
    sent, kept, matrix = build_both(
        core,
        chunk,
        rows // PROJ,
        scaling,
        kpoint,
        species,
        counts,
        miller_index,
        flat,
        positions,
        radial,
        by_atom,
    )
    come = lax.ppermute(sent[0], CORE, swap)
    summed = (kept[0] + come).astype(jnp.bfloat16).reshape(near, rows, 2 * bands)
    exchange = functools.partial(lax.all_to_all, split_axis=0, concat_axis=0, tiled=True)
    parts = exchange(summed, NEAR, axis_index_groups=near_groups)
    parts = exchange(fold(parts, far), FAR, axis_index_groups=far_groups)
    mine = weigh(parts, matrix, near)
    own = exchange(mine, NEAR, axis_index_groups=near_groups)
    other = lax.ppermute(own, CORE, swap)
    estimate = pl.CostEstimate(
        flops=4 * slots * planes * bands, bytes_accessed=4 * 1024 * 1024, transcendentals=0
    )
    params = pltpu.CompilerParams(vmem_limit_bytes=32 * 1024 * 1024)
    total = pl.pallas_call(
        first_kernel,
        out_shape=jax.ShapeDtypeStruct((2 * bands, planes), jnp.float32),
        in_specs=[vmem] * 3,
        out_specs=vmem,
        cost_estimate=estimate,
        compiler_params=params,
        name="spread_own",
    )(own, *kept[1:])
    applied, energy = pl.pallas_call(
        functools.partial(last_kernel, float(slots)),
        out_shape=(
            jax.ShapeDtypeStruct((2 * bands, planes), jnp.bfloat16),
            jax.ShapeDtypeStruct((1, bands), jnp.float32),
        ),
        in_specs=[vmem] * 5,
        out_specs=(vmem, vmem),
        cost_estimate=estimate,
        compiler_params=params,
        name="spread_other",
    )(own, other, *sent[1:3], total)
    return applied.reshape(2, bands, planes), energy.reshape(bands)


def solution(mesh):
    split = Mesh(
        mesh.devices.reshape(mesh.shape["kpt"], 4, 16, 2), ("kpt", *GA)
    )
    in_specs = (P(None, GA), P("kpt"), P(None, "kpt", GA), P(), P(), P(), P(), P())
    out_specs = (P(None, "kpt", GA), P("kpt"))
    return jax.shard_map(
        on_device, mesh=split, in_specs=in_specs, out_specs=out_specs, check_vma=False
    )
```

```python
import functools
import math

import jax
import jax.numpy as jnp
import numpy as np
from jax import lax
from jax.experimental import pallas as pl
from jax.experimental.pallas import tpu as pltpu
from jax.sharding import Mesh
from jax.sharding import PartitionSpec as P

PROJ = 8
MGRID = 64
GA = ("x", "z", "c")
NEAR = ("x", "z")
FAR = "z"
CORE = "c"
EXTRA = 8
SMALL = 8 * 1024 * 1024


def groups_of(wide, ring, span=4):
    blocks = ring // span
    inner = [*range(1, span - 1), 0, span - 1]
    turn = [span // 2 if 2 * b >= blocks else 0 for b in range(blocks)]
    place = [[b * span + (q + turn[b]) % span for q in inner] for b in range(blocks)]
    near = [[w * ring + z for w in range(wide) for z in place[b]] for b in range(blocks)]
    late = [*range(blocks // 2, blocks), *range(blocks // 2)]
    far = [[place[b][q] for b in late] for q in range(span)]
    return near, far


def rank_along(z, ring, span=4):
    q = lax.rem(z + jnp.where(2 * z >= ring, span // 2, 0), span)
    return jnp.where(q == 0, span - 2, jnp.where(q == span - 1, span - 1, q - 1))


def turn_series(degree=6):
    nodes = 0.125 + 0.125 * np.cos(np.pi * (np.arange(64) + 0.5) / 64)
    root = np.sqrt(nodes)
    fit = np.polynomial.chebyshev.Chebyshev.fit
    poly = np.polynomial.Polynomial
    cosine = fit(nodes, np.cos(2 * np.pi * root), degree, domain=[0, 0.25]).convert(kind=poly)
    sine = fit(nodes, np.sin(2 * np.pi * root) / root, degree, domain=[0, 0.25]).convert(kind=poly)
    return [float(v) for v in cosine.coef], [float(v) for v in sine.coef]


COSINE, SINE = turn_series()


def series(coefficients, y):
    total = jnp.full_like(y, coefficients[-1])
    for value in coefficients[-2::-1]:
        total = total * y + value
    return total


def nearest(x):
    return jnp.floor(x + 0.5)


def fill(first, amp_ref, cos_ref, sin_ref, species_ref, counts_ref, real_ref, imag_ref, per=8):
    atoms, planes = sin_ref.shape
    slot = lax.broadcasted_iota(jnp.int32, (PROJ, planes), 0)

    def step(index, carry):
        real, imag = [], []
        for k in range(per):
            at = index * per + k
            kind = species_ref[first + at]
            number = counts_ref[first + at]
            amp = amp_ref[pl.ds(pl.multiple_of(kind * PROJ, PROJ), PROJ), :]
            amp = jnp.where(slot < number, amp, 0.0)
            real.append(amp * cos_ref[pl.ds(at, 1), :])
            imag.append(amp * sin_ref[pl.ds(at, 1), :])
        rows = pl.ds(pl.multiple_of(index * per * PROJ, per * PROJ), per * PROJ)
        real_ref[rows, :] = jnp.concatenate(real, 0).astype(jnp.bfloat16)
        imag_ref[rows, :] = jnp.concatenate(imag, 0).astype(jnp.bfloat16)
        return carry

    lax.fori_loop(0, atoms // per, step, 0)


def wave_pair(turns):
    turns = turns - nearest(turns)
    square = turns * turns
    return series(COSINE, square), series(SINE, square) * -turns


def overlap(real_ref, imag_ref, waves):
    bands = waves.shape[0] // 2
    turned = jnp.concatenate([waves[bands:], -waves[:bands]], 0)
    outer = (((1,), (1,)), ((), ()))
    return lax.dot_general(
        real_ref[...], waves, outer, preferred_element_type=jnp.float32
    ) + lax.dot_general(imag_ref[...], turned, outer, preferred_element_type=jnp.float32)


def send_kernel(
    scaling,
    chunk_atoms,
    half_ref,
    chunk_ref,
    kpoint_hbm,
    species_hbm,
    counts_hbm,
    miller_hbm,
    waves_hbm,
    positions_hbm,
    radial_hbm,
    coupling_hbm,
    over_ref,
    real_ref,
    imag_ref,
    amp_ref,
    rest_ref,
    waves_ref,
    species_out,
    counts_out,
    matrix_ref,
    all_ref,
    cos_ref,
    sin_ref,
    kpoint_ref,
    species_ref,
    counts_ref,
    miller_ref,
    positions_ref,
    radial_ref,
    coupling_ref,
    done,
):
    f32, bf16 = jnp.float32, jnp.bfloat16
    pairs = (
        (miller_hbm, miller_ref),
        (kpoint_hbm, kpoint_ref),
        (radial_hbm, radial_ref),
        (positions_hbm, positions_ref),
        (species_hbm, species_ref),
        (counts_hbm, counts_ref),
        (species_hbm, species_out),
        (counts_hbm, counts_out),
        (coupling_hbm, coupling_ref),
        (waves_hbm, waves_ref),
    )
    copies = [pltpu.make_async_copy(a, b, done.at[i]) for i, (a, b) in enumerate(pairs)]
    for copy in copies:
        copy.start()
    terms = radial_ref.shape[1]
    planes = miller_ref.shape[1]
    atoms = sin_ref.shape[0]
    kinds = radial_ref.shape[0] // PROJ
    half = half_ref[0]
    for copy in copies[:-4]:
        copy.wait()

    miller = miller_ref[...].astype(f32)
    shifted = [miller[c : c + 1] + kpoint_ref[c] for c in range(3)]
    squared = shifted[0] * shifted[0] + shifted[1] * shifted[1] + shifted[2] * shifted[2]
    order = lax.broadcasted_iota(jnp.int32, (terms, planes), 0)
    widths = jnp.zeros((terms, planes), f32)
    for r in range(terms):
        widths = jnp.where(order == r, 0.001 * 1.5**r, widths)
    basis = jnp.exp(-widths * squared)
    radial = jnp.dot(
        radial_ref[...], basis, precision=lax.Precision.HIGHEST, preferred_element_type=f32
    )
    scale = 1.0 / jnp.sqrt(squared + 1.0)
    row = lax.broadcasted_iota(jnp.int32, (PROJ, planes), 0) % 4
    angular = jnp.where(row == 0, 1.0, jnp.where(row == 1, shifted[0] * scale, 0.0))
    angular = jnp.where(row == 2, shifted[1] * scale, angular)
    angular = jnp.where(row == 3, shifted[2] * scale, angular) * scaling
    for s in range(kinds):
        amp_ref[s * PROJ : (s + 1) * PROJ, :] = radial[s * PROJ : (s + 1) * PROJ] * angular

    places = positions_ref[...].astype(f32)
    third = lax.broadcasted_iota(jnp.int32, (3, 128), 0)
    point = jnp.where(third == 0, kpoint_ref[0], jnp.where(third == 1, kpoint_ref[1], kpoint_ref[2]))
    inner = (((0,), (0,)), ((), ()))
    winding = lax.dot_general(
        places.astype(bf16), miller.astype(bf16), inner, preferred_element_type=f32
    )
    offset = lax.dot_general(
        places, point, inner, precision=lax.Precision.HIGHEST, preferred_element_type=f32
    )
    winding = winding * (1.0 / MGRID)
    offset = offset * (1.0 / MGRID)
    winding = winding - nearest(winding)
    offset = offset - nearest(offset)
    all_ref[...] = winding + jnp.concatenate([offset] * (planes // 128), 1)
    first = pl.multiple_of(half * atoms, atoms)
    other = pl.multiple_of((1 - half) * atoms, atoms)
    rest_ref[...] = all_ref[pl.ds(other, atoms), :]
    cosine, sine = wave_pair(all_ref[pl.ds(first, atoms), :])
    cos_ref[...] = cosine
    sin_ref[...] = sine
    fill(first, amp_ref, cos_ref, sin_ref, species_ref, counts_ref, real_ref, imag_ref)
    for copy in copies[-4:]:
        copy.wait()
    lanes = coupling_ref.shape[1]
    matrix_ref[...] = pltpu.roll(coupling_ref[...], lanes - chunk_ref[0] * chunk_atoms, 1)
    over_ref[...] = overlap(real_ref, imag_ref, waves_ref[...])


def keep_kernel(
    half_ref,
    species_vmem,
    counts_vmem,
    amp_ref,
    turns_ref,
    waves_ref,
    over_ref,
    real_ref,
    imag_ref,
    cos_ref,
    sin_ref,
    species_ref,
    counts_ref,
    done,
):
    copies = [
        pltpu.make_async_copy(species_vmem, species_ref, done.at[0]),
        pltpu.make_async_copy(counts_vmem, counts_ref, done.at[1]),
    ]
    for copy in copies:
        copy.start()
    cosine, sine = wave_pair(turns_ref[...])
    cos_ref[...] = cosine
    sin_ref[...] = sine
    for copy in copies:
        copy.wait()
    first = half_ref[0] * cos_ref.shape[0]
    fill(first, amp_ref, cos_ref, sin_ref, species_ref, counts_ref, real_ref, imag_ref)
    over_ref[...] = overlap(real_ref, imag_ref, waves_ref[...])


def build_both(core, chunk, chunk_atoms, scaling, kpoint, species, counts, miller, waves, positions, radial, coupling):
    planes = miller.shape[1]
    atoms = species.shape[0] // 2
    slots = atoms * PROJ
    smem = pl.BlockSpec(memory_space=pltpu.SMEM)
    vmem = pl.BlockSpec(memory_space=pltpu.VMEM)
    hbm = pl.BlockSpec(memory_space=pltpu.HBM)
    shape = jax.ShapeDtypeStruct
    whole = [kpoint, species, counts, miller, waves, positions, radial, coupling]
    whole = [pltpu.with_memory_space_constraint(a, pltpu.HBM) for a in whole]
    results = (
        shape((slots, waves.shape[0]), jnp.float32),
        shape((slots, planes), jnp.bfloat16),
        shape((slots, planes), jnp.bfloat16),
    )
    waving = [pltpu.VMEM((atoms, planes), jnp.float32)] * 2
    tables = [pltpu.SMEM(species.shape, species.dtype), pltpu.SMEM(counts.shape, counts.dtype)]
    estimate = pl.CostEstimate(
        flops=4 * slots * planes * waves.shape[0], bytes_accessed=2**22, transcendentals=0
    )
    params = pltpu.CompilerParams(vmem_limit_bytes=32 * 1024 * 1024)
    *sent, amp, turns, held, kinds, numbers, matrix = pl.pallas_call(
        functools.partial(send_kernel, scaling, chunk_atoms),
        out_shape=(
            *results,
            shape((radial.shape[0], planes), jnp.float32),
            shape((atoms, planes), jnp.float32),
            shape(waves.shape, waves.dtype),
            shape(species.shape, species.dtype),
            shape(counts.shape, counts.dtype),
            shape(coupling.shape, coupling.dtype),
        ),
        in_specs=[smem] * 2 + [hbm] * 8,
        out_specs=(vmem,) * 9,
        scratch_shapes=[
            pltpu.VMEM((2 * atoms, planes), jnp.float32),
            *waving,
            pltpu.SMEM(kpoint.shape, kpoint.dtype),
            *tables,
            pltpu.VMEM(miller.shape, miller.dtype),
            pltpu.VMEM(positions.shape, positions.dtype),
            pltpu.VMEM(radial.shape, radial.dtype),
            pltpu.VMEM(coupling.shape, coupling.dtype),
            pltpu.SemaphoreType.DMA((10,)),
        ],
        cost_estimate=estimate,
        compiler_params=params,
        name="build_send",
    )((1 - core).reshape(1), chunk.reshape(1), *whole)
    kept = pl.pallas_call(
        keep_kernel,
        out_shape=results,
        in_specs=[smem] + [vmem] * 5,
        out_specs=(vmem,) * 3,
        scratch_shapes=[*waving, *tables, pltpu.SemaphoreType.DMA((2,))],
        cost_estimate=estimate,
        compiler_params=params,
        name="build_keep",
    )(core.reshape(1), kinds, numbers, amp, turns, held)
    return sent, kept, matrix


def fold_kernel(parts_ref, out_ref):
    total = jnp.sum(parts_ref[...].astype(jnp.float32), axis=0).astype(out_ref.dtype)
    for k in range(out_ref.shape[0]):
        out_ref[k] = total


def fold(parts, copies):
    return pl.pallas_call(
        fold_kernel,
        out_shape=pltpu.VMEM((copies, *parts.shape[1:]), parts.dtype),
        in_specs=[pl.BlockSpec(memory_space=pltpu.VMEM)],
        out_specs=pl.BlockSpec(memory_space=pltpu.VMEM),
        compiler_params=pltpu.CompilerParams(vmem_limit_bytes=SMALL),
        name="fold",
    )(parts)


def weigh_kernel(parts_ref, matrix_ref, out_ref):
    f32, bf16 = jnp.float32, jnp.bfloat16
    over = jnp.sum(parts_ref[...].astype(f32), axis=0)
    rows, both = over.shape
    bands = both // 2
    weighted = []
    for k in range(rows // PROJ):
        block = over[k * PROJ : (k + 1) * PROJ]
        total = 0.0
        for j in range(PROJ):
            total = total + matrix_ref[j * PROJ : (j + 1) * PROJ, k : k + 1] * block[j : j + 1]
        weighted.append(total)
    weighted = jnp.concatenate(weighted, 0)
    energy = jnp.sum(over * weighted, axis=0, keepdims=True)
    energy = energy[:, :bands] + energy[:, bands:]
    high = energy.astype(bf16).astype(f32)
    index = lax.broadcasted_iota(jnp.int32, (EXTRA, bands), 0)
    share = jnp.where(index == 0, high, jnp.where(index == 1, energy - high, 0.0))
    whole = jnp.concatenate([weighted[:, :bands], weighted[:, bands:], share], 0).astype(bf16)
    for k in range(out_ref.shape[0]):
        out_ref[k] = whole


def weigh(parts, matrix, copies):
    rows, both = parts.shape[1:]
    vmem = pl.BlockSpec(memory_space=pltpu.VMEM)
    return pl.pallas_call(
        weigh_kernel,
        out_shape=jax.ShapeDtypeStruct((copies, 2 * rows + EXTRA, both // 2), jnp.bfloat16),
        in_specs=[vmem, vmem],
        out_specs=vmem,
        compiler_params=pltpu.CompilerParams(vmem_limit_bytes=SMALL),
        name="weigh",
    )(parts, matrix)


def spread(table_ref, real_ref, imag_ref):
    copies, rows, bands = table_ref.shape
    rows = (rows - EXTRA) // 2
    real = table_ref[:, 0:rows, :].reshape(copies * rows, bands)
    imag = table_ref[:, rows : 2 * rows, :].reshape(copies * rows, bands)
    real, imag = jnp.transpose(real), jnp.transpose(imag)
    table = jnp.concatenate([real, imag], 0)
    turned = jnp.concatenate([-imag, real], 0)
    return jnp.dot(table, real_ref[...], preferred_element_type=jnp.float32) + jnp.dot(
        turned, imag_ref[...], preferred_element_type=jnp.float32
    )


def share_of(table_ref):
    rows = table_ref.shape[1] - EXTRA
    return jnp.sum(table_ref[:, rows:, :].astype(jnp.float32), axis=(0, 1), keepdims=True)[0]


def first_kernel(table_ref, real_ref, imag_ref, out_ref):
    out_ref[...] = spread(table_ref, real_ref, imag_ref)


def last_kernel(slots, own_ref, table_ref, real_ref, imag_ref, total_ref, out_ref, energy_ref):
    out_ref[...] = (total_ref[...] + spread(table_ref, real_ref, imag_ref)).astype(out_ref.dtype)
    energy_ref[...] = (share_of(own_ref) + share_of(table_ref)) / slots


def on_device(miller_index, kpoint, waves, species, counts, positions, radial_coef, coupling):
    planes = waves.shape[2]
    bands = waves.shape[1]
    scaling = 1.0 / math.sqrt(planes * lax.axis_size(GA))
    slots = coupling.shape[0] * PROJ
    near_groups, far_groups = groups_of(lax.axis_size("x"), lax.axis_size("z"))
    near, far = len(near_groups[0]), len(far_groups[0])
    rows = slots // (2 * near)
    core = lax.axis_index(CORE)
    rank = rank_along(lax.axis_index("z"), lax.axis_size("z"))
    chunk = core * near + lax.axis_index("x") * len(far_groups) + rank
    vmem = pl.BlockSpec(memory_space=pltpu.VMEM)
    swap = [(0, 1), (1, 0)]
    flat = waves.reshape(2 * bands, planes)
    radial = radial_coef.reshape(-1, radial_coef.shape[2])
    by_atom = jnp.transpose(coupling, (1, 2, 0)).reshape(PROJ * PROJ, -1)
    sent, kept, matrix = build_both(
        core,
        chunk,
        rows // PROJ,
        scaling,
        kpoint,
        species,
        counts,
        miller_index,
        flat,
        positions,
        radial,
        by_atom,
    )
    come = lax.ppermute(sent[0], CORE, swap)
    summed = (kept[0] + come).astype(jnp.bfloat16).reshape(near, rows, 2 * bands)
    exchange = functools.partial(lax.all_to_all, split_axis=0, concat_axis=0, tiled=True)
    parts = exchange(summed, NEAR, axis_index_groups=near_groups)
    parts = exchange(fold(parts, far), FAR, axis_index_groups=far_groups)
    mine = weigh(parts, matrix, near)
    own = exchange(mine, NEAR, axis_index_groups=near_groups)
    other = lax.ppermute(own, CORE, swap)
    estimate = pl.CostEstimate(
        flops=4 * slots * planes * bands, bytes_accessed=4 * 1024 * 1024, transcendentals=0
    )
    params = pltpu.CompilerParams(vmem_limit_bytes=32 * 1024 * 1024)
    total = pl.pallas_call(
        first_kernel,
        out_shape=jax.ShapeDtypeStruct((2 * bands, planes), jnp.float32),
        in_specs=[vmem] * 3,
        out_specs=vmem,
        cost_estimate=estimate,
        compiler_params=params,
        name="spread_own",
    )(own, *kept[1:])
    applied, energy = pl.pallas_call(
        functools.partial(last_kernel, float(slots)),
        out_shape=(
            jax.ShapeDtypeStruct((2 * bands, planes), jnp.bfloat16),
            jax.ShapeDtypeStruct((1, bands), jnp.float32),
        ),
        in_specs=[vmem] * 5,
        out_specs=(vmem, vmem),
        cost_estimate=estimate,
        compiler_params=params,
        name="spread_other",
    )(own, other, *sent[1:3], total)
    return applied.reshape(2, bands, planes), energy.reshape(bands)


def solution(mesh):
    split = Mesh(
        mesh.devices.reshape(mesh.shape["kpt"], 4, 16, 2), ("kpt", *GA)
    )
    in_specs = (P(None, GA), P("kpt"), P(None, "kpt", GA), P(), P(), P(), P(), P())
    out_specs = (P(None, "kpt", GA), P("kpt"))
    return jax.shard_map(
        on_device, mesh=split, in_specs=in_specs, out_specs=out_specs, check_vma=False
    )
```

```python
import functools
import math

import jax
import jax.numpy as jnp
import numpy as np
from jax import lax
from jax.experimental import pallas as pl
from jax.experimental.pallas import tpu as pltpu
from jax.sharding import Mesh
from jax.sharding import PartitionSpec as P

PROJ = 8
MGRID = 64
GA = ("x", "z", "c")
NEAR = ("x", "z")
FAR = "z"
CORE = "c"
EXTRA = 8
SMALL = 8 * 1024 * 1024


def groups_of(wide, ring, span=4):
    blocks = ring // span
    inner = [*range(1, span - 1), 0, span - 1]
    turn = [span // 2 if 2 * b >= blocks else 0 for b in range(blocks)]
    place = [[b * span + (q + turn[b]) % span for q in inner] for b in range(blocks)]
    near = [
        [(w + 1) % wide * ring + z for w in range(wide) for z in place[b]] for b in range(blocks)
    ]
    late = [*reversed(range(blocks // 2, blocks)), *range(blocks // 2)]
    far = [[place[b][q] for b in late] for q in range(span)]
    return near, far


def rank_along(z, ring, span=4):
    q = lax.rem(z + jnp.where(2 * z >= ring, span // 2, 0), span)
    return jnp.where(q == 0, span - 2, jnp.where(q == span - 1, span - 1, q - 1))


def turn_series(degree=6):
    nodes = 0.125 + 0.125 * np.cos(np.pi * (np.arange(64) + 0.5) / 64)
    root = np.sqrt(nodes)
    fit = np.polynomial.chebyshev.Chebyshev.fit
    poly = np.polynomial.Polynomial
    cosine = fit(nodes, np.cos(2 * np.pi * root), degree, domain=[0, 0.25]).convert(kind=poly)
    sine = fit(nodes, np.sin(2 * np.pi * root) / root, degree, domain=[0, 0.25]).convert(kind=poly)
    return [float(v) for v in cosine.coef], [float(v) for v in sine.coef]


COSINE, SINE = turn_series()


def series(coefficients, y):
    total = jnp.full_like(y, coefficients[-1])
    for value in coefficients[-2::-1]:
        total = total * y + value
    return total


def nearest(x):
    return jnp.floor(x + 0.5)


def fill(first, amp_ref, cos_ref, sin_ref, species_ref, counts_ref, real_ref, imag_ref, per=8):
    atoms, planes = sin_ref.shape
    slot = lax.broadcasted_iota(jnp.int32, (PROJ, planes), 0)

    def step(index, carry):
        real, imag = [], []
        for k in range(per):
            at = index * per + k
            kind = species_ref[first + at]
            number = counts_ref[first + at]
            amp = amp_ref[pl.ds(pl.multiple_of(kind * PROJ, PROJ), PROJ), :]
            amp = jnp.where(slot < number, amp, 0.0)
            real.append(amp * cos_ref[pl.ds(at, 1), :])
            imag.append(amp * sin_ref[pl.ds(at, 1), :])
        rows = pl.ds(pl.multiple_of(index * per * PROJ, per * PROJ), per * PROJ)
        real_ref[rows, :] = jnp.concatenate(real, 0).astype(jnp.bfloat16)
        imag_ref[rows, :] = jnp.concatenate(imag, 0).astype(jnp.bfloat16)
        return carry

    lax.fori_loop(0, atoms // per, step, 0)


def wave_pair(turns):
    turns = turns - nearest(turns)
    square = turns * turns
    return series(COSINE, square), series(SINE, square) * -turns


def overlap(real_ref, imag_ref, waves):
    bands = waves.shape[0] // 2
    turned = jnp.concatenate([waves[bands:], -waves[:bands]], 0)
    outer = (((1,), (1,)), ((), ()))
    return lax.dot_general(
        real_ref[...], waves, outer, preferred_element_type=jnp.float32
    ) + lax.dot_general(imag_ref[...], turned, outer, preferred_element_type=jnp.float32)


def send_kernel(
    scaling,
    chunk_atoms,
    half_ref,
    chunk_ref,
    kpoint_hbm,
    species_hbm,
    counts_hbm,
    miller_hbm,
    waves_hbm,
    positions_hbm,
    radial_hbm,
    coupling_hbm,
    over_ref,
    real_ref,
    imag_ref,
    amp_ref,
    rest_ref,
    waves_ref,
    species_out,
    counts_out,
    matrix_ref,
    all_ref,
    cos_ref,
    sin_ref,
    kpoint_ref,
    species_ref,
    counts_ref,
    miller_ref,
    positions_ref,
    radial_ref,
    coupling_ref,
    done,
):
    f32, bf16 = jnp.float32, jnp.bfloat16
    pairs = (
        (miller_hbm, miller_ref),
        (kpoint_hbm, kpoint_ref),
        (radial_hbm, radial_ref),
        (positions_hbm, positions_ref),
        (species_hbm, species_ref),
        (counts_hbm, counts_ref),
        (species_hbm, species_out),
        (counts_hbm, counts_out),
        (coupling_hbm, coupling_ref),
        (waves_hbm, waves_ref),
    )
    copies = [pltpu.make_async_copy(a, b, done.at[i]) for i, (a, b) in enumerate(pairs)]
    for copy in copies:
        copy.start()
    terms = radial_ref.shape[1]
    planes = miller_ref.shape[1]
    atoms = sin_ref.shape[0]
    kinds = radial_ref.shape[0] // PROJ
    half = half_ref[0]
    for copy in copies[:-4]:
        copy.wait()

    miller = miller_ref[...].astype(f32)
    shifted = [miller[c : c + 1] + kpoint_ref[c] for c in range(3)]
    squared = shifted[0] * shifted[0] + shifted[1] * shifted[1] + shifted[2] * shifted[2]
    order = lax.broadcasted_iota(jnp.int32, (terms, planes), 0)
    widths = jnp.zeros((terms, planes), f32)
    for r in range(terms):
        widths = jnp.where(order == r, 0.001 * 1.5**r, widths)
    basis = jnp.exp(-widths * squared)
    radial = jnp.dot(
        radial_ref[...], basis, precision=lax.Precision.HIGHEST, preferred_element_type=f32
    )
    scale = 1.0 / jnp.sqrt(squared + 1.0)
    row = lax.broadcasted_iota(jnp.int32, (PROJ, planes), 0) % 4
    angular = jnp.where(row == 0, 1.0, jnp.where(row == 1, shifted[0] * scale, 0.0))
    angular = jnp.where(row == 2, shifted[1] * scale, angular)
    angular = jnp.where(row == 3, shifted[2] * scale, angular) * scaling
    for s in range(kinds):
        amp_ref[s * PROJ : (s + 1) * PROJ, :] = radial[s * PROJ : (s + 1) * PROJ] * angular

    places = positions_ref[...].astype(f32)
    third = lax.broadcasted_iota(jnp.int32, (3, 128), 0)
    point = jnp.where(third == 0, kpoint_ref[0], jnp.where(third == 1, kpoint_ref[1], kpoint_ref[2]))
    inner = (((0,), (0,)), ((), ()))
    winding = lax.dot_general(
        places.astype(bf16), miller.astype(bf16), inner, preferred_element_type=f32
    )
    offset = lax.dot_general(
        places, point, inner, precision=lax.Precision.HIGHEST, preferred_element_type=f32
    )
    winding = winding * (1.0 / MGRID)
    offset = offset * (1.0 / MGRID)
    winding = winding - nearest(winding)
    offset = offset - nearest(offset)
    all_ref[...] = winding + jnp.concatenate([offset] * (planes // 128), 1)
    first = pl.multiple_of(half * atoms, atoms)
    other = pl.multiple_of((1 - half) * atoms, atoms)
    rest_ref[...] = all_ref[pl.ds(other, atoms), :]
    cosine, sine = wave_pair(all_ref[pl.ds(first, atoms), :])
    cos_ref[...] = cosine
    sin_ref[...] = sine
    fill(first, amp_ref, cos_ref, sin_ref, species_ref, counts_ref, real_ref, imag_ref)
    for copy in copies[-4:]:
        copy.wait()
    lanes = coupling_ref.shape[1]
    matrix_ref[...] = pltpu.roll(coupling_ref[...], lanes - chunk_ref[0] * chunk_atoms, 1)
    over_ref[...] = overlap(real_ref, imag_ref, waves_ref[...])


def keep_kernel(
    half_ref,
    species_vmem,
    counts_vmem,
    amp_ref,
    turns_ref,
    waves_ref,
    over_ref,
    real_ref,
    imag_ref,
    cos_ref,
    sin_ref,
    species_ref,
    counts_ref,
    done,
):
    copies = [
        pltpu.make_async_copy(species_vmem, species_ref, done.at[0]),
        pltpu.make_async_copy(counts_vmem, counts_ref, done.at[1]),
    ]
    for copy in copies:
        copy.start()
    cosine, sine = wave_pair(turns_ref[...])
    cos_ref[...] = cosine
    sin_ref[...] = sine
    for copy in copies:
        copy.wait()
    first = half_ref[0] * cos_ref.shape[0]
    fill(first, amp_ref, cos_ref, sin_ref, species_ref, counts_ref, real_ref, imag_ref)
    over_ref[...] = overlap(real_ref, imag_ref, waves_ref[...])


def build_both(core, chunk, chunk_atoms, scaling, kpoint, species, counts, miller, waves, positions, radial, coupling):
    planes = miller.shape[1]
    atoms = species.shape[0] // 2
    slots = atoms * PROJ
    smem = pl.BlockSpec(memory_space=pltpu.SMEM)
    vmem = pl.BlockSpec(memory_space=pltpu.VMEM)
    hbm = pl.BlockSpec(memory_space=pltpu.HBM)
    shape = jax.ShapeDtypeStruct
    whole = [kpoint, species, counts, miller, waves, positions, radial, coupling]
    whole = [pltpu.with_memory_space_constraint(a, pltpu.HBM) for a in whole]
    results = (
        shape((slots, waves.shape[0]), jnp.float32),
        shape((slots, planes), jnp.bfloat16),
        shape((slots, planes), jnp.bfloat16),
    )
    waving = [pltpu.VMEM((atoms, planes), jnp.float32)] * 2
    tables = [pltpu.SMEM(species.shape, species.dtype), pltpu.SMEM(counts.shape, counts.dtype)]
    estimate = pl.CostEstimate(
        flops=4 * slots * planes * waves.shape[0], bytes_accessed=2**22, transcendentals=0
    )
    params = pltpu.CompilerParams(vmem_limit_bytes=32 * 1024 * 1024)
    *sent, amp, turns, held, kinds, numbers, matrix = pl.pallas_call(
        functools.partial(send_kernel, scaling, chunk_atoms),
        out_shape=(
            *results,
            shape((radial.shape[0], planes), jnp.float32),
            shape((atoms, planes), jnp.float32),
            shape(waves.shape, waves.dtype),
            shape(species.shape, species.dtype),
            shape(counts.shape, counts.dtype),
            shape(coupling.shape, coupling.dtype),
        ),
        in_specs=[smem] * 2 + [hbm] * 8,
        out_specs=(vmem,) * 9,
        scratch_shapes=[
            pltpu.VMEM((2 * atoms, planes), jnp.float32),
            *waving,
            pltpu.SMEM(kpoint.shape, kpoint.dtype),
            *tables,
            pltpu.VMEM(miller.shape, miller.dtype),
            pltpu.VMEM(positions.shape, positions.dtype),
            pltpu.VMEM(radial.shape, radial.dtype),
            pltpu.VMEM(coupling.shape, coupling.dtype),
            pltpu.SemaphoreType.DMA((10,)),
        ],
        cost_estimate=estimate,
        compiler_params=params,
        name="build_send",
    )((1 - core).reshape(1), chunk.reshape(1), *whole)
    kept = pl.pallas_call(
        keep_kernel,
        out_shape=results,
        in_specs=[smem] + [vmem] * 5,
        out_specs=(vmem,) * 3,
        scratch_shapes=[*waving, *tables, pltpu.SemaphoreType.DMA((2,))],
        cost_estimate=estimate,
        compiler_params=params,
        name="build_keep",
    )(core.reshape(1), kinds, numbers, amp, turns, held)
    return sent, kept, matrix


def fold_kernel(parts_ref, out_ref):
    total = jnp.sum(parts_ref[...].astype(jnp.float32), axis=0).astype(out_ref.dtype)
    for k in range(out_ref.shape[0]):
        out_ref[k] = total


def fold(parts, copies):
    return pl.pallas_call(
        fold_kernel,
        out_shape=pltpu.VMEM((copies, *parts.shape[1:]), parts.dtype),
        in_specs=[pl.BlockSpec(memory_space=pltpu.VMEM)],
        out_specs=pl.BlockSpec(memory_space=pltpu.VMEM),
        compiler_params=pltpu.CompilerParams(vmem_limit_bytes=SMALL),
        name="fold",
    )(parts)


def weigh_kernel(parts_ref, matrix_ref, out_ref):
    f32, bf16 = jnp.float32, jnp.bfloat16
    over = jnp.sum(parts_ref[...].astype(f32), axis=0)
    rows, both = over.shape
    bands = both // 2
    weighted = []
    for k in range(rows // PROJ):
        block = over[k * PROJ : (k + 1) * PROJ]
        total = 0.0
        for j in range(PROJ):
            total = total + matrix_ref[j * PROJ : (j + 1) * PROJ, k : k + 1] * block[j : j + 1]
        weighted.append(total)
    weighted = jnp.concatenate(weighted, 0)
    energy = jnp.sum(over * weighted, axis=0, keepdims=True)
    energy = energy[:, :bands] + energy[:, bands:]
    high = energy.astype(bf16).astype(f32)
    index = lax.broadcasted_iota(jnp.int32, (EXTRA, bands), 0)
    share = jnp.where(index == 0, high, jnp.where(index == 1, energy - high, 0.0))
    whole = jnp.concatenate([weighted[:, :bands], weighted[:, bands:], share], 0).astype(bf16)
    for k in range(out_ref.shape[0]):
        out_ref[k] = whole


def weigh(parts, matrix, copies):
    rows, both = parts.shape[1:]
    vmem = pl.BlockSpec(memory_space=pltpu.VMEM)
    return pl.pallas_call(
        weigh_kernel,
        out_shape=jax.ShapeDtypeStruct((copies, 2 * rows + EXTRA, both // 2), jnp.bfloat16),
        in_specs=[vmem, vmem],
        out_specs=vmem,
        compiler_params=pltpu.CompilerParams(vmem_limit_bytes=SMALL),
        name="weigh",
    )(parts, matrix)


def spread(table_ref, real_ref, imag_ref):
    copies, rows, bands = table_ref.shape
    rows = (rows - EXTRA) // 2
    real = table_ref[:, 0:rows, :].reshape(copies * rows, bands)
    imag = table_ref[:, rows : 2 * rows, :].reshape(copies * rows, bands)
    real, imag = jnp.transpose(real), jnp.transpose(imag)
    table = jnp.concatenate([real, imag], 0)
    turned = jnp.concatenate([-imag, real], 0)
    return jnp.dot(table, real_ref[...], preferred_element_type=jnp.float32) + jnp.dot(
        turned, imag_ref[...], preferred_element_type=jnp.float32
    )


def share_of(table_ref):
    rows = table_ref.shape[1] - EXTRA
    return jnp.sum(table_ref[:, rows:, :].astype(jnp.float32), axis=(0, 1), keepdims=True)[0]


def first_kernel(table_ref, real_ref, imag_ref, out_ref):
    out_ref[...] = spread(table_ref, real_ref, imag_ref)


def last_kernel(slots, own_ref, table_ref, real_ref, imag_ref, total_ref, out_ref, energy_ref):
    out_ref[...] = (total_ref[...] + spread(table_ref, real_ref, imag_ref)).astype(out_ref.dtype)
    energy_ref[...] = (share_of(own_ref) + share_of(table_ref)) / slots


def on_device(miller_index, kpoint, waves, species, counts, positions, radial_coef, coupling):
    planes = waves.shape[2]
    bands = waves.shape[1]
    scaling = 1.0 / math.sqrt(planes * lax.axis_size(GA))
    slots = coupling.shape[0] * PROJ
    near_groups, far_groups = groups_of(lax.axis_size("x"), lax.axis_size("z"))
    near, far = len(near_groups[0]), len(far_groups[0])
    rows = slots // (2 * near)
    core = lax.axis_index(CORE)
    rank = rank_along(lax.axis_index("z"), lax.axis_size("z"))
    wide = lax.axis_size("x")
    across = lax.rem(lax.axis_index("x") + wide - 1, wide)
    chunk = core * near + across * len(far_groups) + rank
    vmem = pl.BlockSpec(memory_space=pltpu.VMEM)
    swap = [(0, 1), (1, 0)]
    flat = waves.reshape(2 * bands, planes)
    radial = radial_coef.reshape(-1, radial_coef.shape[2])
    by_atom = jnp.transpose(coupling, (1, 2, 0)).reshape(PROJ * PROJ, -1)
    sent, kept, matrix = build_both(
        core,
        chunk,
        rows // PROJ,
        scaling,
        kpoint,
        species,
        counts,
        miller_index,
        flat,
        positions,
        radial,
        by_atom,
    )
    come = lax.ppermute(sent[0], CORE, swap)
    summed = (kept[0] + come).astype(jnp.bfloat16).reshape(near, rows, 2 * bands)
    exchange = functools.partial(lax.all_to_all, split_axis=0, concat_axis=0, tiled=True)
    parts = exchange(summed, NEAR, axis_index_groups=near_groups)
    parts = exchange(fold(parts, far), FAR, axis_index_groups=far_groups)
    mine = weigh(parts, matrix, near)
    own = exchange(mine, NEAR, axis_index_groups=near_groups)
    other = lax.ppermute(own, CORE, swap)
    estimate = pl.CostEstimate(
        flops=4 * slots * planes * bands, bytes_accessed=4 * 1024 * 1024, transcendentals=0
    )
    params = pltpu.CompilerParams(vmem_limit_bytes=32 * 1024 * 1024)
    total = pl.pallas_call(
        first_kernel,
        out_shape=jax.ShapeDtypeStruct((2 * bands, planes), jnp.float32),
        in_specs=[vmem] * 3,
        out_specs=vmem,
        cost_estimate=estimate,
        compiler_params=params,
        name="spread_own",
    )(own, *kept[1:])
    applied, energy = pl.pallas_call(
        functools.partial(last_kernel, float(slots)),
        out_shape=(
            jax.ShapeDtypeStruct((2 * bands, planes), jnp.bfloat16),
            jax.ShapeDtypeStruct((1, bands), jnp.float32),
        ),
        in_specs=[vmem] * 5,
        out_specs=(vmem, vmem),
        cost_estimate=estimate,
        compiler_params=params,
        name="spread_other",
    )(own, other, *sent[1:3], total)
    return applied.reshape(2, bands, planes), energy.reshape(bands)


def solution(mesh):
    split = Mesh(
        mesh.devices.reshape(mesh.shape["kpt"], 4, 16, 2), ("kpt", *GA)
    )
    in_specs = (P(None, GA), P("kpt"), P(None, "kpt", GA), P(), P(), P(), P(), P())
    out_specs = (P(None, "kpt", GA), P("kpt"))
    return jax.shard_map(
        on_device, mesh=split, in_specs=in_specs, out_specs=out_specs, check_vma=False
    )
```

```python
import functools
import math

import jax
import jax.numpy as jnp
import numpy as np
from jax import lax
from jax.experimental import pallas as pl
from jax.experimental.pallas import tpu as pltpu
from jax.sharding import Mesh
from jax.sharding import PartitionSpec as P

PROJ = 8
MGRID = 64
GA = ("x", "z", "c")
NEAR = ("x", "z")
FAR = "z"
CORE = "c"
EXTRA = 8
SMALL = 8 * 1024 * 1024


def groups_of(wide, ring, span=4):
    blocks = ring // span
    inner = [*range(1, span - 1), 0, span - 1]
    turn = [span // 2 if 2 * b >= blocks else 0 for b in range(blocks)]
    place = [[b * span + (q + turn[b]) % span for q in inner] for b in range(blocks)]
    near = [
        [(w + 1) % wide * ring + z for w in range(wide) for z in place[b]] for b in range(blocks)
    ]
    far = [[place[b][q] for b in reversed(range(blocks))] for q in range(span)]
    return near, far


def rank_along(z, ring, span=4):
    q = lax.rem(z + jnp.where(2 * z >= ring, span // 2, 0), span)
    return jnp.where(q == 0, span - 2, jnp.where(q == span - 1, span - 1, q - 1))


def turn_series(degree=6):
    nodes = 0.125 + 0.125 * np.cos(np.pi * (np.arange(64) + 0.5) / 64)
    root = np.sqrt(nodes)
    fit = np.polynomial.chebyshev.Chebyshev.fit
    poly = np.polynomial.Polynomial
    cosine = fit(nodes, np.cos(2 * np.pi * root), degree, domain=[0, 0.25]).convert(kind=poly)
    sine = fit(nodes, np.sin(2 * np.pi * root) / root, degree, domain=[0, 0.25]).convert(kind=poly)
    return [float(v) for v in cosine.coef], [float(v) for v in sine.coef]


COSINE, SINE = turn_series()


def series(coefficients, y):
    total = jnp.full_like(y, coefficients[-1])
    for value in coefficients[-2::-1]:
        total = total * y + value
    return total


def nearest(x):
    return jnp.floor(x + 0.5)


def fill(first, amp_ref, cos_ref, sin_ref, species_ref, counts_ref, real_ref, imag_ref, per=8):
    atoms, planes = sin_ref.shape
    slot = lax.broadcasted_iota(jnp.int32, (PROJ, planes), 0)

    def step(index, carry):
        real, imag = [], []
        for k in range(per):
            at = index * per + k
            kind = species_ref[first + at]
            number = counts_ref[first + at]
            amp = amp_ref[pl.ds(pl.multiple_of(kind * PROJ, PROJ), PROJ), :]
            amp = jnp.where(slot < number, amp, 0.0)
            real.append(amp * cos_ref[pl.ds(at, 1), :])
            imag.append(amp * sin_ref[pl.ds(at, 1), :])
        rows = pl.ds(pl.multiple_of(index * per * PROJ, per * PROJ), per * PROJ)
        real_ref[rows, :] = jnp.concatenate(real, 0).astype(jnp.bfloat16)
        imag_ref[rows, :] = jnp.concatenate(imag, 0).astype(jnp.bfloat16)
        return carry

    lax.fori_loop(0, atoms // per, step, 0)


def wave_pair(turns):
    turns = turns - nearest(turns)
    square = turns * turns
    return series(COSINE, square), series(SINE, square) * -turns


def overlap(real_ref, imag_ref, waves):
    bands = waves.shape[0] // 2
    turned = jnp.concatenate([waves[bands:], -waves[:bands]], 0)
    outer = (((1,), (1,)), ((), ()))
    return lax.dot_general(
        real_ref[...], waves, outer, preferred_element_type=jnp.float32
    ) + lax.dot_general(imag_ref[...], turned, outer, preferred_element_type=jnp.float32)


def send_kernel(
    scaling,
    chunk_atoms,
    half_ref,
    chunk_ref,
    kpoint_hbm,
    species_hbm,
    counts_hbm,
    miller_hbm,
    waves_hbm,
    positions_hbm,
    radial_hbm,
    coupling_hbm,
    over_ref,
    real_ref,
    imag_ref,
    amp_ref,
    rest_ref,
    waves_ref,
    species_out,
    counts_out,
    matrix_ref,
    all_ref,
    cos_ref,
    sin_ref,
    kpoint_ref,
    species_ref,
    counts_ref,
    miller_ref,
    positions_ref,
    radial_ref,
    coupling_ref,
    done,
):
    f32, bf16 = jnp.float32, jnp.bfloat16
    pairs = (
        (miller_hbm, miller_ref),
        (kpoint_hbm, kpoint_ref),
        (radial_hbm, radial_ref),
        (positions_hbm, positions_ref),
        (species_hbm, species_ref),
        (counts_hbm, counts_ref),
        (species_hbm, species_out),
        (counts_hbm, counts_out),
        (coupling_hbm, coupling_ref),
        (waves_hbm, waves_ref),
    )
    copies = [pltpu.make_async_copy(a, b, done.at[i]) for i, (a, b) in enumerate(pairs)]
    for copy in copies:
        copy.start()
    terms = radial_ref.shape[1]
    planes = miller_ref.shape[1]
    atoms = sin_ref.shape[0]
    kinds = radial_ref.shape[0] // PROJ
    half = half_ref[0]
    for copy in copies[:-4]:
        copy.wait()

    miller = miller_ref[...].astype(f32)
    shifted = [miller[c : c + 1] + kpoint_ref[c] for c in range(3)]
    squared = shifted[0] * shifted[0] + shifted[1] * shifted[1] + shifted[2] * shifted[2]
    order = lax.broadcasted_iota(jnp.int32, (terms, planes), 0)
    widths = jnp.zeros((terms, planes), f32)
    for r in range(terms):
        widths = jnp.where(order == r, 0.001 * 1.5**r, widths)
    basis = jnp.exp(-widths * squared)
    radial = jnp.dot(
        radial_ref[...], basis, precision=lax.Precision.HIGHEST, preferred_element_type=f32
    )
    scale = 1.0 / jnp.sqrt(squared + 1.0)
    row = lax.broadcasted_iota(jnp.int32, (PROJ, planes), 0) % 4
    angular = jnp.where(row == 0, 1.0, jnp.where(row == 1, shifted[0] * scale, 0.0))
    angular = jnp.where(row == 2, shifted[1] * scale, angular)
    angular = jnp.where(row == 3, shifted[2] * scale, angular) * scaling
    for s in range(kinds):
        amp_ref[s * PROJ : (s + 1) * PROJ, :] = radial[s * PROJ : (s + 1) * PROJ] * angular

    places = positions_ref[...].astype(f32)
    third = lax.broadcasted_iota(jnp.int32, (3, 128), 0)
    point = jnp.where(third == 0, kpoint_ref[0], jnp.where(third == 1, kpoint_ref[1], kpoint_ref[2]))
    inner = (((0,), (0,)), ((), ()))
    winding = lax.dot_general(
        places.astype(bf16), miller.astype(bf16), inner, preferred_element_type=f32
    )
    offset = lax.dot_general(
        places, point, inner, precision=lax.Precision.HIGHEST, preferred_element_type=f32
    )
    winding = winding * (1.0 / MGRID)
    offset = offset * (1.0 / MGRID)
    winding = winding - nearest(winding)
    offset = offset - nearest(offset)
    all_ref[...] = winding + jnp.concatenate([offset] * (planes // 128), 1)
    first = pl.multiple_of(half * atoms, atoms)
    other = pl.multiple_of((1 - half) * atoms, atoms)
    rest_ref[...] = all_ref[pl.ds(other, atoms), :]
    cosine, sine = wave_pair(all_ref[pl.ds(first, atoms), :])
    cos_ref[...] = cosine
    sin_ref[...] = sine
    fill(first, amp_ref, cos_ref, sin_ref, species_ref, counts_ref, real_ref, imag_ref)
    for copy in copies[-4:]:
        copy.wait()
    lanes = coupling_ref.shape[1]
    matrix_ref[...] = pltpu.roll(coupling_ref[...], lanes - chunk_ref[0] * chunk_atoms, 1)
    over_ref[...] = overlap(real_ref, imag_ref, waves_ref[...])


def keep_kernel(
    half_ref,
    species_vmem,
    counts_vmem,
    amp_ref,
    turns_ref,
    waves_ref,
    over_ref,
    real_ref,
    imag_ref,
    cos_ref,
    sin_ref,
    species_ref,
    counts_ref,
    done,
):
    copies = [
        pltpu.make_async_copy(species_vmem, species_ref, done.at[0]),
        pltpu.make_async_copy(counts_vmem, counts_ref, done.at[1]),
    ]
    for copy in copies:
        copy.start()
    cosine, sine = wave_pair(turns_ref[...])
    cos_ref[...] = cosine
    sin_ref[...] = sine
    for copy in copies:
        copy.wait()
    first = half_ref[0] * cos_ref.shape[0]
    fill(first, amp_ref, cos_ref, sin_ref, species_ref, counts_ref, real_ref, imag_ref)
    over_ref[...] = overlap(real_ref, imag_ref, waves_ref[...])


def build_both(core, chunk, chunk_atoms, scaling, kpoint, species, counts, miller, waves, positions, radial, coupling):
    planes = miller.shape[1]
    atoms = species.shape[0] // 2
    slots = atoms * PROJ
    smem = pl.BlockSpec(memory_space=pltpu.SMEM)
    vmem = pl.BlockSpec(memory_space=pltpu.VMEM)
    hbm = pl.BlockSpec(memory_space=pltpu.HBM)
    shape = jax.ShapeDtypeStruct
    whole = [kpoint, species, counts, miller, waves, positions, radial, coupling]
    whole = [pltpu.with_memory_space_constraint(a, pltpu.HBM) for a in whole]
    results = (
        shape((slots, waves.shape[0]), jnp.float32),
        shape((slots, planes), jnp.bfloat16),
        shape((slots, planes), jnp.bfloat16),
    )
    waving = [pltpu.VMEM((atoms, planes), jnp.float32)] * 2
    tables = [pltpu.SMEM(species.shape, species.dtype), pltpu.SMEM(counts.shape, counts.dtype)]
    estimate = pl.CostEstimate(
        flops=4 * slots * planes * waves.shape[0], bytes_accessed=2**22, transcendentals=0
    )
    params = pltpu.CompilerParams(vmem_limit_bytes=32 * 1024 * 1024)
    *sent, amp, turns, held, kinds, numbers, matrix = pl.pallas_call(
        functools.partial(send_kernel, scaling, chunk_atoms),
        out_shape=(
            *results,
            shape((radial.shape[0], planes), jnp.float32),
            shape((atoms, planes), jnp.float32),
            shape(waves.shape, waves.dtype),
            shape(species.shape, species.dtype),
            shape(counts.shape, counts.dtype),
            shape(coupling.shape, coupling.dtype),
        ),
        in_specs=[smem] * 2 + [hbm] * 8,
        out_specs=(vmem,) * 9,
        scratch_shapes=[
            pltpu.VMEM((2 * atoms, planes), jnp.float32),
            *waving,
            pltpu.SMEM(kpoint.shape, kpoint.dtype),
            *tables,
            pltpu.VMEM(miller.shape, miller.dtype),
            pltpu.VMEM(positions.shape, positions.dtype),
            pltpu.VMEM(radial.shape, radial.dtype),
            pltpu.VMEM(coupling.shape, coupling.dtype),
            pltpu.SemaphoreType.DMA((10,)),
        ],
        cost_estimate=estimate,
        compiler_params=params,
        name="build_send",
    )((1 - core).reshape(1), chunk.reshape(1), *whole)
    kept = pl.pallas_call(
        keep_kernel,
        out_shape=results,
        in_specs=[smem] + [vmem] * 5,
        out_specs=(vmem,) * 3,
        scratch_shapes=[*waving, *tables, pltpu.SemaphoreType.DMA((2,))],
        cost_estimate=estimate,
        compiler_params=params,
        name="build_keep",
    )(core.reshape(1), kinds, numbers, amp, turns, held)
    return sent, kept, matrix


def fold_kernel(parts_ref, out_ref):
    total = jnp.sum(parts_ref[...].astype(jnp.float32), axis=0).astype(out_ref.dtype)
    for k in range(out_ref.shape[0]):
        out_ref[k] = total


def fold(parts, copies):
    return pl.pallas_call(
        fold_kernel,
        out_shape=pltpu.VMEM((copies, *parts.shape[1:]), parts.dtype),
        in_specs=[pl.BlockSpec(memory_space=pltpu.VMEM)],
        out_specs=pl.BlockSpec(memory_space=pltpu.VMEM),
        compiler_params=pltpu.CompilerParams(vmem_limit_bytes=SMALL),
        name="fold",
    )(parts)


def weigh_kernel(parts_ref, matrix_ref, out_ref):
    f32, bf16 = jnp.float32, jnp.bfloat16
    over = jnp.sum(parts_ref[...].astype(f32), axis=0)
    rows, both = over.shape
    bands = both // 2
    weighted = []
    for k in range(rows // PROJ):
        block = over[k * PROJ : (k + 1) * PROJ]
        total = 0.0
        for j in range(PROJ):
            total = total + matrix_ref[j * PROJ : (j + 1) * PROJ, k : k + 1] * block[j : j + 1]
        weighted.append(total)
    weighted = jnp.concatenate(weighted, 0)
    energy = jnp.sum(over * weighted, axis=0, keepdims=True)
    energy = energy[:, :bands] + energy[:, bands:]
    high = energy.astype(bf16).astype(f32)
    index = lax.broadcasted_iota(jnp.int32, (EXTRA, bands), 0)
    share = jnp.where(index == 0, high, jnp.where(index == 1, energy - high, 0.0))
    whole = jnp.concatenate([weighted[:, :bands], weighted[:, bands:], share], 0).astype(bf16)
    for k in range(out_ref.shape[0]):
        out_ref[k] = whole


def weigh(parts, matrix, copies):
    rows, both = parts.shape[1:]
    vmem = pl.BlockSpec(memory_space=pltpu.VMEM)
    return pl.pallas_call(
        weigh_kernel,
        out_shape=jax.ShapeDtypeStruct((copies, 2 * rows + EXTRA, both // 2), jnp.bfloat16),
        in_specs=[vmem, vmem],
        out_specs=vmem,
        compiler_params=pltpu.CompilerParams(vmem_limit_bytes=SMALL),
        name="weigh",
    )(parts, matrix)


def spread(table_ref, real_ref, imag_ref):
    copies, rows, bands = table_ref.shape
    rows = (rows - EXTRA) // 2
    real = table_ref[:, 0:rows, :].reshape(copies * rows, bands)
    imag = table_ref[:, rows : 2 * rows, :].reshape(copies * rows, bands)
    real, imag = jnp.transpose(real), jnp.transpose(imag)
    table = jnp.concatenate([real, imag], 0)
    turned = jnp.concatenate([-imag, real], 0)
    return jnp.dot(table, real_ref[...], preferred_element_type=jnp.float32) + jnp.dot(
        turned, imag_ref[...], preferred_element_type=jnp.float32
    )


def share_of(table_ref):
    rows = table_ref.shape[1] - EXTRA
    return jnp.sum(table_ref[:, rows:, :].astype(jnp.float32), axis=(0, 1), keepdims=True)[0]


def first_kernel(table_ref, real_ref, imag_ref, out_ref):
    out_ref[...] = spread(table_ref, real_ref, imag_ref)


def last_kernel(slots, own_ref, table_ref, real_ref, imag_ref, total_ref, out_ref, energy_ref):
    out_ref[...] = (total_ref[...] + spread(table_ref, real_ref, imag_ref)).astype(out_ref.dtype)
    energy_ref[...] = (share_of(own_ref) + share_of(table_ref)) / slots


def on_device(miller_index, kpoint, waves, species, counts, positions, radial_coef, coupling):
    planes = waves.shape[2]
    bands = waves.shape[1]
    scaling = 1.0 / math.sqrt(planes * lax.axis_size(GA))
    slots = coupling.shape[0] * PROJ
    near_groups, far_groups = groups_of(lax.axis_size("x"), lax.axis_size("z"))
    near, far = len(near_groups[0]), len(far_groups[0])
    rows = slots // (2 * near)
    core = lax.axis_index(CORE)
    rank = rank_along(lax.axis_index("z"), lax.axis_size("z"))
    wide = lax.axis_size("x")
    across = lax.rem(lax.axis_index("x") + wide - 1, wide)
    chunk = core * near + across * len(far_groups) + rank
    vmem = pl.BlockSpec(memory_space=pltpu.VMEM)
    swap = [(0, 1), (1, 0)]
    flat = waves.reshape(2 * bands, planes)
    radial = radial_coef.reshape(-1, radial_coef.shape[2])
    by_atom = jnp.transpose(coupling, (1, 2, 0)).reshape(PROJ * PROJ, -1)
    sent, kept, matrix = build_both(
        core,
        chunk,
        rows // PROJ,
        scaling,
        kpoint,
        species,
        counts,
        miller_index,
        flat,
        positions,
        radial,
        by_atom,
    )
    come = lax.ppermute(sent[0], CORE, swap)
    summed = (kept[0] + come).astype(jnp.bfloat16).reshape(near, rows, 2 * bands)
    exchange = functools.partial(lax.all_to_all, split_axis=0, concat_axis=0, tiled=True)
    parts = exchange(summed, NEAR, axis_index_groups=near_groups)
    parts = exchange(fold(parts, far), FAR, axis_index_groups=far_groups)
    mine = weigh(parts, matrix, near)
    own = exchange(mine, NEAR, axis_index_groups=near_groups)
    other = lax.ppermute(own, CORE, swap)
    estimate = pl.CostEstimate(
        flops=4 * slots * planes * bands, bytes_accessed=4 * 1024 * 1024, transcendentals=0
    )
    params = pltpu.CompilerParams(vmem_limit_bytes=32 * 1024 * 1024)
    total = pl.pallas_call(
        first_kernel,
        out_shape=jax.ShapeDtypeStruct((2 * bands, planes), jnp.float32),
        in_specs=[vmem] * 3,
        out_specs=vmem,
        cost_estimate=estimate,
        compiler_params=params,
        name="spread_own",
    )(own, *kept[1:])
    applied, energy = pl.pallas_call(
        functools.partial(last_kernel, float(slots)),
        out_shape=(
            jax.ShapeDtypeStruct((2 * bands, planes), jnp.bfloat16),
            jax.ShapeDtypeStruct((1, bands), jnp.float32),
        ),
        in_specs=[vmem] * 5,
        out_specs=(vmem, vmem),
        cost_estimate=estimate,
        compiler_params=params,
        name="spread_other",
    )(own, other, *sent[1:3], total)
    return applied.reshape(2, bands, planes), energy.reshape(bands)


def solution(mesh):
    split = Mesh(
        mesh.devices.reshape(mesh.shape["kpt"], 4, 16, 2), ("kpt", *GA)
    )
    in_specs = (P(None, GA), P("kpt"), P(None, "kpt", GA), P(), P(), P(), P(), P())
    out_specs = (P(None, "kpt", GA), P("kpt"))
    return jax.shard_map(
        on_device, mesh=split, in_specs=in_specs, out_specs=out_specs, check_vma=False
    )
```
